32 devices in a mesh: dp: 1, tp: 32 (over x, y, z, core).
Axes of the slice: x: 2, y: 2, z: 4, core: 2. Of those that a mesh axis runs over, the one named last changes fastest.
Arguments:
- x: bfloat16 [2048, 12288], P('dp')
- w_gate: bfloat16 [12288, 28672], P(None, 'tp')
- w_up: bfloat16 [12288, 28672], P(None, 'tp')
- w_down: bfloat16 [28672, 12288], P('tp')
Outputs:
- output: bfloat16 [2048, 12288], P('dp')
All inputs are finite; a program needn't handle non-finite values.
Results may differ from the reference program's by a relative error of at most 0.016.
Values are sent between devices in bfloat16 or wider.
A program may use at most 2 GiB of HBM per device.

```python
import jax
import jax.numpy as jnp

ROWS = 2048
D = 12288
FF = 28672


def setup_inputs(seed: int = 0, part: int = 0) -> dict:
    kx, kg, ku, kd = jax.random.split(jax.random.key(seed), 4)
    drawn = {
        "x": jax.random.normal(jax.random.fold_in(kx, part), (ROWS, D), jnp.float32),
        "w_gate": jax.random.normal(kg, (D, FF), jnp.float32) * D**-0.5,
        "w_up": jax.random.normal(ku, (D, FF), jnp.float32) * D**-0.5,
        "w_down": jax.random.normal(kd, (FF, D), jnp.float32) * FF**-0.5,
    }
    return {k: v.astype(jnp.bfloat16) for k, v in drawn.items()}


def reference(x, w_gate, w_up, w_down):
    gate = jnp.dot(x, w_gate, preferred_element_type=jnp.float32)
    up = jnp.dot(x, w_up, preferred_element_type=jnp.float32)
    hidden = (jax.nn.silu(gate) * up).astype(jnp.bfloat16)
    return jnp.dot(hidden, w_down, preferred_element_type=jnp.float32).astype(jnp.bfloat16)
```

```python
import functools

import jax
import jax.numpy as jnp
from jax import lax
from jax.experimental import pallas as pl
from jax.experimental.pallas import tpu as pltpu
from jax.sharding import PartitionSpec as P

F32 = jnp.float32
BF16 = jnp.bfloat16
MESH = pl.DeviceIdType.MESH


def dims(rows, d, ff, chunk, pieces):
    wa = d // 24
    return dict(n=rows // chunk, R=chunk, D=d, FF=ff, WA=wa, H=wa // 2, WB=wa // 4, NK=pieces, KB=d // pieces)


def body(cfg, x_ref, wg_ref, wu_ref, wdh_ref, ta, tb, wd, h, xb, wgb, wub, accg, accu, ps, pr, a2s, a2r, a3s, a3r, t1s, t1r, t2s, t2r,
         b1s, b1r, b2s, b2r, b3s, b3r, b4s, b4r, b5s, b5r, fa, fb,
         wd_m, g_m, p_s, p_m, a2_s, a2_m, a3_s, a3_m, t1_s, t1_m, t2_s, t2_m, b1_s, b1_m, b2_s, b2_m, b3_s, b3_m, b4_s, b4_m, b5_s, b5_m,
         la_m, lb_m, fa_s, fb_s, q_s, g1_m, g2_m, g3_m, g4_m, g5_m, h1_m, h2_m, hz_m, h5_m,
         cp, ca2, ca3, ct1, ct2, cb1, cb2, cb3, cb4, cb5):
    n, R, D, WA, H, WB, NK, KB = (cfg[k] for k in ("n", "R", "D", "WA", "H", "WB", "NK", "KB"))
    NB = xb.shape[0]
    me = lax.axis_index("tp")
    dp = lax.axis_index("dp")
    x, y, z, c = me // 16, (me // 8) % 2, (me // 2) % 4, me % 2

    def dev(x, y, z, c):
        return (dp, ((x * 2 + y) * 4 + z) * 2 + c)

    outer = (z == 0) | (z == 3)
    inner = jnp.logical_not(outer)
    up_ok, dn_ok = z < 3, z > 0
    zu, zd = jnp.minimum(z + 1, 3), jnp.maximum(z - 1, 0)
    zin = jnp.where(outer, jnp.where(z == 0, 1, 2), 3 - z)
    zout = jnp.where(z < 2, 0, 3)
    near = jnp.where(z < 2, 0, 1)
    far = 1 - near
    partner = dev(x, y, z, 1 - c)
    xn, yn = dev(1 - x, y, z, c), dev(x, 1 - y, z, c)
    up, down, zin_d, zout_d = dev(x, y, zu, c), dev(x, y, zd, c), dev(x, y, zin, c), dev(x, y, zout, c)
    go, gx, gy, gd = x * 2 + y, (1 - x) * 2 + y, x * 2 + 1 - y, (1 - x) * 2 + 1 - y

    def pick(order, a, b):
        first = order == 0
        return jax.tree.map(lambda p, q: jnp.where(first, p, q), a, b)

    def fn(order):
        return pick(order, xn, yn)

    def sn(order):
        return pick(order, yn, xn)

    def gf(order):
        return pick(order, gx, gy)

    def gs(order):
        return pick(order, gy, gx)

    def copy(src, dst, ss, rs, to):
        return pltpu.make_async_remote_copy(src, dst, ss, rs, device_id=to, device_id_type=MESH)

    def signal(sem, to):
        pl.semaphore_signal(sem, inc=1, device_id=to, device_id_type=MESH)

    def col_a(core, order, g, half=0):
        return core * (8 * WA) + order * (4 * WA) + g * WA + half * H

    def col_b(core, q, g=0):
        return 16 * WA + core * (16 * WB) + q * (4 * WB) + g * WB

    def lanes(i, w):
        return pl.ds(pl.multiple_of(i * w, w), w)

    def dot(i, col, w, unit):
        return jnp.dot(h[i % 3], wd[:, pl.ds(pl.multiple_of(col, unit), w)], preferred_element_type=F32)

    def c_p(s):
        return copy(ps, pr.at[s], p_s, p_m.at[s], partner)

    def c_a2(s, o, m):
        return copy(a2s.at[o, m], a2r.at[s, o, m], a2_s.at[o, m], a2_m.at[s, o, m], fn(o))

    def c_a3(s, o):
        return copy(a3s.at[o], a3r.at[s, o], a3_s.at[o], a3_m.at[s, o], sn(o))

    def c_t1(o):
        return copy(t1s.at[o], t1r.at[o], t1_s.at[o], t1_m.at[o], zin_d)

    def c_t2(src, o):
        return copy(t2s.at[o], t2r.at[src, o], t2_s.at[o], t2_m.at[src, o], zin_d)

    def c_b1():
        return copy(b1s, b1r, b1_s, b1_m, zin_d)

    def c_b2(d):
        return copy(b2s, b2r.at[d], b2_s, b2_m.at[d], zin_d)

    def c_b3(d, to=up):
        return copy(b3s.at[d], b3r.at[d], b3_s.at[d], b3_m.at[d], to)

    def c_b4(o, m):
        return copy(b4s.at[m], b4r.at[m], b4_s.at[m], b4_m.at[m], fn(o))

    def c_b5(o):
        return copy(b5s, b5r, b5_s, b5_m, sn(o))

    def g_copies(kk):
        i, k, b = kk // NK, kk % NK, kk % NB
        rows, ks = pl.ds(pl.multiple_of(i * R, R), R), pl.ds(pl.multiple_of(k * KB, KB), KB)
        return (pltpu.make_async_copy(x_ref.at[rows, ks], xb.at[b], g_m.at[b, 0]),
                pltpu.make_async_copy(wg_ref.at[ks], wgb.at[b], g_m.at[b, 1]),
                pltpu.make_async_copy(wu_ref.at[ks], wub.at[b], g_m.at[b, 2]))

    def g_pieces(i, k0, k1):
        def step(k, _):
            kk = i * NK + k
            b = kk % NB
            for cp_ in g_copies(kk):
                cp_.wait()

            @pl.when(kk + NB - 1 < n * NK)
            def _():
                for cp_ in g_copies(kk + NB - 1):
                    cp_.start()

            @pl.when(k == 0)
            def _():
                accg[...] = jnp.zeros_like(accg)
                accu[...] = jnp.zeros_like(accu)

            accg[...] += jnp.dot(xb[b], wgb[b], preferred_element_type=F32)
            accu[...] += jnp.dot(xb[b], wub[b], preferred_element_type=F32)
            return 0

        lax.fori_loop(k0, k1, step, 0)
        if k1 == NK:
            h[i % 3] = (jax.nn.silu(accg[...]) * accu[...]).astype(BF16)

    def s1(t):
        @pl.when(t >= 1)
        def _():
            c_p(0).wait_send()

        @pl.when(t >= 2)
        def _():
            pl.semaphore_wait(cp, 1)

        def step(j, _):
            col = jnp.where(j < 8, col_a(1 - c, 0, j), col_b(1 - c, j - 8))
            ps[j] = dot(t, col, WA, WA).astype(BF16)
            copy(ps.at[j], pr.at[t % 2, j], p_s, p_m.at[t % 2], partner).start()
            return 0

        lax.fori_loop(0, 12, step, 0)

    def s2(t, m):
        def step(o, _):
            @pl.when(t >= 1)
            def _():
                c_a2(0, o, m).wait_send()

            if m == 0:
                @pl.when(t >= 2)
                def _():
                    pl.semaphore_wait(ca2.at[o], 1)

            g = gf(o) if m else gd
            v = dot(t, col_a(c, o, g), WA, WA) + pr[t % 2, o * 4 + g].astype(F32)
            a2s[o, m] = v.astype(BF16)
            c_a2(t % 2, o, m).start()
            return 0

        lax.fori_loop(0, 2, step, 0)

    def s3(t):
        def step(o, _):
            @pl.when(t >= 1)
            def _():
                c_a3(0, o).wait_send()

            @pl.when(t >= 2)
            def _():
                pl.semaphore_wait(ca3.at[o], 1)

            c_a2(t % 2, o, 0).wait_recv()
            g = gs(o)
            v = dot(t, col_a(c, o, g), WA, WA) + pr[t % 2, o * 4 + g].astype(F32) + a2r[t % 2, o, 0].astype(F32)
            a3s[o] = v.astype(BF16)
            c_a3(t % 2, o).start()
            return 0

        lax.fori_loop(0, 2, step, 0)

    def t1(t):
        c_p(t % 2).wait_recv()

        @pl.when(outer)
        def _():
            @pl.when(t >= 1)
            def _():
                c_b1().wait_send()
                pl.semaphore_wait(cb1, 1)

            q = 3 - z
            b1s[...] = (dot(t, col_b(c, q), WA, WA) + pr[t % 2, 8 + q].astype(F32)).astype(BF16)
            c_b1().start()

    def t2(t):
        @pl.when(t >= 1)
        def _():
            c_b2(0).wait_send()
            pl.semaphore_wait(cb2, 1)

        @pl.when(inner)
        def _():
            c_b1().wait_recv()

        q = (z + 2) % 4
        b2s[...] = (dot(t, col_b(c, q), WA, WA) + pr[t % 2, 8 + q].astype(F32) + b1r[...].astype(F32)).astype(BF16)
        d = jnp.where(z < 2, 0, 1)
        c_b2(d).start()

        @pl.when(inner & (t + 1 < n))
        def _():
            signal(cb1, zout_d)

    def s4(u):
        for o in range(2):
            c_a3(u % 2, o).wait_recv()
            c_a2(u % 2, o, 1).wait_recv()

        @pl.when(outer)
        def _():
            def step(o, _):
                @pl.when(u >= 1)
                def _():
                    c_t1(o).wait_send()

                @pl.when((u >= 1) & (o == 0))
                def _():
                    pl.semaphore_wait(ct1, 1)

                t1s[o] = own_a(u, o, far).astype(BF16)
                c_t1(o).start()
                return 0

            lax.fori_loop(0, 2, step, 0)

    def own_a(u, o, half):
        s, ln = u % 2, lanes(half, H)
        return (dot(u, col_a(c, o, go, half), H, H) + pr[s, o * 4 + go, :, ln].astype(F32)
                + a2r[s, o, 1, :, ln].astype(F32) + a3r[s, o, :, ln].astype(F32))

    def s5(u):
        src = jnp.where(outer, 0, 1)

        def step(o, _):
            @pl.when(u >= 1)
            def _():
                c_t2(src, o).wait_send()

            @pl.when((u >= 1) & (o == 0))
            def _():
                pl.semaphore_wait(ct2, 1)

            @pl.when(inner)
            def _():
                c_t1(o).wait_recv()

            half = jnp.where(outer, near, far)
            t2s[o] = (own_a(u, o, half) + t1r[o].astype(F32)).astype(BF16)
            c_t2(src, o).start()
            return 0

        lax.fori_loop(0, 2, step, 0)

        @pl.when(inner & (u + 1 < n))
        def _():
            signal(ct1, zout_d)

    def win_a(u, o, g, half):
        return ta.at[u, c, o, g, half]

    def fa_copies(u, o):
        w = win_a(u, o, go, near)
        f = fa.at[o]
        return ((f, w, fa_s.at[o, 0], g1_m.at[u], zout_d), (f, w, fa_s.at[o, 1], g1_m.at[u], zin_d),
                (f, w, fa_s.at[o, 2], g3_m.at[0, u], sn(o)), (f, w, fa_s.at[o, 3], g4_m.at[0, u], fn(o)),
                (f, w, fa_s.at[o, 4], g5_m.at[u], partner))

    def fa_done(u, o):
        for a in fa_copies(u, o):
            copy(*a).wait_send()
        pltpu.make_async_copy(fa.at[o], win_a(u, o, go, near), la_m.at[o]).wait()

    def s6(u):
        @pl.when(inner)
        def _():
            for o in range(2):
                for src in range(2):
                    c_t2(src, o).wait_recv()

            def step(o, _):
                @pl.when(u >= 1)
                def _():
                    fa_done(u, o)

                fa[o] = (own_a(u, o, near) + t2r[0, o].astype(F32) + t2r[1, o].astype(F32)).astype(BF16)
                pltpu.make_async_copy(fa.at[o], win_a(u, o, go, near), la_m.at[o]).start()
                for a in fa_copies(u, o):
                    copy(*a).start()
                return 0

            lax.fori_loop(0, 2, step, 0)

            @pl.when(u + 1 < n)
            def _():
                signal(ct2, zout_d)
                signal(ct2, zin_d)

        @pl.when(u + 2 < n)
        def _():
            for o in range(2):
                signal(ca2.at[o], fn(o))
                signal(ca3.at[o], sn(o))

    def t3(u):
        def step(d, _):
            ok = jnp.where(d == 0, up_ok, dn_ok)

            @pl.when(ok)
            def _():
                to = pick(d, up, down)

                @pl.when(u >= 1)
                def _():
                    c_b3(d, to).wait_send()
                    pl.semaphore_wait(cb3.at[d], 1)

                @pl.when(inner)
                def _():
                    c_b2(d).wait_recv()

                q = pick(d, zu, zd)
                b3s[d] = (dot(u, col_b(c, q), WA, WA) + pr[u % 2, 8 + q].astype(F32) + b2r[d].astype(F32)).astype(BF16)
                c_b3(d, to).start()

            return 0

        lax.fori_loop(0, 2, step, 0)

        @pl.when(inner & (u + 1 < n))
        def _():
            signal(cb2, zout_d)
            signal(cb2, zin_d)

    def own_b(u, g):
        ln = lanes(g, WB)
        return (dot(u, col_b(c, z, g), WB, WB) + pr[u % 2, 8 + z, :, ln].astype(F32)
                + b3r[0, :, ln].astype(F32) + b3r[1, :, ln].astype(F32))

    def t4(u):
        @pl.when(dn_ok)
        def _():
            c_b3(0).wait_recv()

        @pl.when(up_ok)
        def _():
            c_b3(1).wait_recv()

        o = u % 2

        def step(m, _):
            @pl.when(u >= 1)
            def _():
                c_b4(o, m).wait_send()

            @pl.when((u >= 1) & (m == 0))
            def _():
                pl.semaphore_wait(cb4, 1)

            b4s[m] = own_b(u, jnp.where(m == 0, gd, gf(o))).astype(BF16)
            c_b4(o, m).start()
            return 0

        lax.fori_loop(0, 2, step, 0)

    def t5(u):
        o = u % 2

        @pl.when(u >= 1)
        def _():
            c_b5(o).wait_send()
            pl.semaphore_wait(cb5, 1)

        c_b4(o, 0).wait_recv()
        b5s[...] = (own_b(u, gs(o)) + b4r[0].astype(F32)).astype(BF16)
        c_b5(o).start()

    def fb_copies(u):
        w, o = tb.at[u, c, z, go], u % 2
        return ((fb, w, fb_s.at[0], h1_m.at[u], sn(o)), (fb, w, fb_s.at[1], h2_m.at[0, u], fn(o)))

    def fb_local(u):
        return pltpu.make_async_copy(fb, tb.at[u, c, z, go], lb_m)

    def t6(u):
        o = u % 2
        c_b4(o, 1).wait_recv()
        c_b5(o).wait_recv()

        @pl.when(u >= 1)
        def _():
            for a in fb_copies(u):
                copy(*a).wait_send()

        fb[...] = (own_b(u, go) + b4r[1].astype(F32) + b5r[...].astype(F32)).astype(BF16)
        fb_local(u).start()
        for a in fb_copies(u):
            copy(*a).start()

        @pl.when(u + 1 < n)
        def _():
            @pl.when(dn_ok)
            def _():
                signal(cb3.at[0], down)

            @pl.when(up_ok)
            def _():
                signal(cb3.at[1], up)

            signal(cb4, fn(1 - o))
            signal(cb5, sn(1 - o))

        @pl.when(u + 2 < n)
        def _():
            signal(cp, partner)

    def go_on(v, cond, k, src, rs, to):
        def make():
            return copy(src(v), src(v), q_s.at[k], rs(v), to)

        @pl.when(cond if cond is not True else v >= 0)
        def _():
            @pl.when(v >= 1)
            def _():
                make().wait_send()

            make().start()

    plan = []

    def op(group, cond, src, rs, to):
        plan.append((group, cond, len(plan), src, rs, to))

    def half_ops(group, cond, half, which):
        for o in range(2):
            w = functools.partial(lambda o, half, v: win_a(v, o, go, half), o, half)
            op(group, cond, w, functools.partial(lambda k, v: g3_m.at[k, v], which), sn(o))
            op(group, cond, w, functools.partial(lambda k, v: g4_m.at[k, v], which), fn(o))
            op(group, cond, w, lambda v: g5_m.at[v], partner)

    for o in range(2):
        op("q0", inner, functools.partial(lambda o, v: win_a(v, o, go, far), o), lambda v: g2_m.at[v], zout_d)
    half_ops("q0i", inner, far, 1)
    half_ops("q0o", outer, near, 0)
    half_ops("q1", outer, far, 1)
    for k, half in ((0, near), (1, far)):
        for o in range(2):
            w = functools.partial(lambda o, half, v: win_a(v, o, gs(o), half), o, half)
            op(f"q{2 + k}", True, w, functools.partial(lambda k, v: g4_m.at[2 + k, v], k), fn(o))
            op(f"q{2 + k}", True, w, lambda v: g5_m.at[v], partner)
    for o in range(2):
        for half in range(2):
            op("q4", True, functools.partial(lambda o, half, v: win_a(v, o, gf(o), half), o, half), lambda v: g5_m.at[v], partner)
            op("q5", True, functools.partial(lambda o, half, v: win_a(v, o, gd, half), o, half), lambda v: g5_m.at[v], partner)
    op("r0", True, lambda v: tb.at[v, c, z, gs(v % 2)], lambda v: h2_m.at[1, v], None)
    block = lambda q: (lambda v: tb.at[v, c, q])
    op("r1", up_ok, block(z), lambda v: hz_m.at[0, v], up)
    op("r1", dn_ok, block(z), lambda v: hz_m.at[1, v], down)
    op("r1", True, block(z), lambda v: h5_m.at[v], partner)
    zm2, zp2 = jnp.maximum(z - 2, 0), jnp.minimum(z + 2, 3)
    op("r2u", dn_ok & up_ok, block(zd), lambda v: hz_m.at[2, v], up)
    op("r2u", dn_ok, block(zd), lambda v: h5_m.at[v], partner)
    op("r2d", dn_ok & up_ok, block(zu), lambda v: hz_m.at[3, v], down)
    op("r2d", up_ok, block(zu), lambda v: h5_m.at[v], partner)
    op("r3u", z == 2, block(zm2), lambda v: hz_m.at[4, v], up)
    op("r3u", z >= 2, block(zm2), lambda v: h5_m.at[v], partner)
    op("r3d", z == 1, block(zp2), lambda v: hz_m.at[5, v], down)
    op("r3d", z <= 1, block(zp2), lambda v: h5_m.at[v], partner)
    op("r4", outer, block(3 - z), lambda v: h5_m.at[v], partner)

    def run(group, v):
        for g_, cond, k, src, rs, to in plan:
            if g_ == group:
                go_on(v, cond, k, src, rs, fn(v % 2) if to is None else to)

    def arrived(ref, sem):
        copy(ref, ref, q_s.at[0], sem, partner).wait_recv()

    def pair(v):
        return ta.at[v, c, :, 0, 0]

    def q0a(v):
        arrived(pair(v), g1_m.at[v])
        run("q0", v)
        run("q0i", v)
        run("q0o", v)

    def q0b(v):
        arrived(tb.at[v, c, 0, 0], h1_m.at[v])
        run("r0", v)

    def q1a(v):
        @pl.when(outer)
        def _():
            arrived(pair(v), g2_m.at[v])

        run("q1", v)

    def q1b(v):
        fb_local(v).wait()
        for k in range(2):
            arrived(tb.at[v, c, 0, 0], h2_m.at[k, v])
        run("r1", v)

    def q2a(v):
        arrived(pair(v), g3_m.at[0, v])
        run("q2", v)

    def q3a(v):
        arrived(pair(v), g3_m.at[1, v])
        run("q3", v)

    def hop(v, up_there, down_there, k, groups):
        for there, kk, g in ((up_there, k, groups[0]), (down_there, k + 1, groups[1])):
            @pl.when(there)
            def _():
                arrived(tb.at[v, c, 0], hz_m.at[kk, v])

            run(g, v)

    def q2b(v):
        hop(v, dn_ok, up_ok, 0, ("r2u", "r2d"))

    def q3b(v):
        hop(v, z >= 2, z <= 1, 2, ("r3u", "r3d"))

    def q4b(v):
        hop(v, z == 3, z == 0, 4, ("", "r4"))

    def q4a(v):
        for k in range(2):
            arrived(pair(v), g4_m.at[k, v])
        run("q4", v)

    def q5(v):
        for k in range(2):
            arrived(pair(v), g4_m.at[2 + k, v])
        run("q5", v)

    @pl.when(outer)
    def _():
        t1r[...] = jnp.zeros_like(t1r)
        b1r[...] = jnp.zeros_like(b1r)
        b2r[...] = jnp.zeros_like(b2r)

    @pl.when(z == 0)
    def _():
        b3r[0] = jnp.zeros_like(b3r[0])

    @pl.when(z == 3)
    def _():
        b3r[1] = jnp.zeros_like(b3r[1])

    for kk in range(NB - 1):
        for cp_ in g_copies(kk):
            cp_.start()

    def wd_copies():
        out = []
        for k, core in enumerate((1 - c, c)):
            for m, (off, w) in enumerate(((col_a(core, 0, 0), 8 * WA), (col_b(core, 0), 16 * WB))):
                cols = pl.ds(pl.multiple_of(off, w), w)
                out.append(pltpu.make_async_copy(wdh_ref.at[:, cols], wd.at[:, cols], wd_m.at[2 * k + m]))
        return out

    g_pieces(0, 0, NK // 2)
    for cp_ in wd_copies():
        cp_.start()
    g_pieces(0, NK // 2, NK)
    cut = [NK * k // 8 for k in range(9)]

    def slot(t, _):
        @pl.when(t == 0)
        def _():
            for cp_ in wd_copies():
                cp_.wait()

        def at(i, f):
            @pl.when((i >= 0) & (i < n))
            def _():
                f(i)

        def g(a, b):
            at(t + 1, lambda i: g_pieces(i, cut[a], cut[b]))

        u, v, w, e = t - 1, t - 2, t - 3, t - 4
        at(u, t3)
        at(t, s1)
        at(w, q2b)
        at(v, q0a)
        at(u, s4)
        g(0, 1)
        at(t, t1)
        at(v, q0b)
        at(u, t4)
        at(t, lambda i: s2(i, 0))
        g(1, 2)
        at(e, q2a)
        at(u, s5)
        at(w, q3a)
        at(w, q3b)
        g(2, 3)
        at(u, t5)
        g(3, 4)
        at(t, lambda i: s2(i, 1))
        at(t, t2)
        at(v, q1b)
        g(4, 5)
        at(t, s3)
        g(5, 7)
        at(u, s6)
        at(u, t6)
        at(e, q4a)
        at(e, q5)
        at(v, q1a)
        g(7, 8)
        at(e, q4b)
        return 0

    lax.fori_loop(0, n + 4, slot, 0)

    last = n - 1
    c_p(0).wait_send()
    for o in range(2):
        for m in range(2):
            c_a2(0, o, m).wait_send()
        c_b4(0, o).wait_send()
        c_a3(0, o).wait_send()
        c_t2(0, o).wait_send()

        @pl.when(outer)
        def _():
            c_t1(o).wait_send()

        @pl.when(inner)
        def _():
            fa_done(last, o)

        @pl.when(up_ok if o == 0 else dn_ok)
        def _():
            c_b3(o).wait_send()

    @pl.when(outer)
    def _():
        c_b1().wait_send()

    c_b2(0).wait_send()
    c_b5(0).wait_send()
    for a in fb_copies(last):
        copy(*a).wait_send()
    for g_, cond, k, src, rs, to in plan:
        def done(k=k, src=src, rs=rs):
            copy(src(last), src(last), q_s.at[k], rs(last), partner).wait_send()

        if cond is True:
            done()
        else:
            pl.when(cond)(done)

    def all_here(v, _):
        arrived(ta.at[v, 1 - c], g5_m.at[v])
        arrived(tb.at[v, 1 - c], h5_m.at[v])
        return 0

    lax.fori_loop(0, n, all_here, 0)


N_OPS = 2 + 6 * 3 + 8 + 8 + 1 + 3 + 8 + 1


def block_sums(cfg, x, w_gate, w_up, w_down):
    n, R, D, FF, WA, H, WB, KB = (cfg[k] for k in ("n", "R", "D", "FF", "WA", "H", "WB", "KB"))
    NB = 4
    vm = lambda *s: pltpu.VMEM(s, BF16)
    dma = lambda *s: pltpu.SemaphoreType.DMA(s) if s else pltpu.SemaphoreType.DMA
    reg = lambda *s: pltpu.SemaphoreType.REGULAR(s) if s else pltpu.SemaphoreType.REGULAR
    scratch = [
        vm(FF, D), vm(3, R, FF), vm(NB, R, KB), vm(NB, KB, FF), vm(NB, KB, FF), pltpu.VMEM((R, FF), F32), pltpu.VMEM((R, FF), F32),
        vm(12, R, WA), vm(2, 12, R, WA), vm(2, 2, R, WA), vm(2, 2, 2, R, WA), vm(2, R, WA), vm(2, 2, R, WA),
        vm(2, R, H), vm(2, R, H), vm(2, R, H), vm(2, 2, R, H),
        vm(R, WA), vm(R, WA), vm(R, WA), vm(2, R, WA), vm(2, R, WA), vm(2, R, WA), vm(2, R, WB), vm(2, R, WB), vm(R, WB), vm(R, WB),
        vm(2, R, H), vm(R, WB),
        dma(4), dma(NB, 3), dma(), dma(2), dma(2, 2), dma(2, 2, 2), dma(2), dma(2, 2), dma(2), dma(2), dma(2), dma(2, 2),
        dma(), dma(), dma(), dma(2), dma(2), dma(2), dma(2), dma(2), dma(), dma(),
        dma(2), dma(), dma(2, 5), dma(2), dma(N_OPS), dma(n), dma(n), dma(2, n), dma(4, n), dma(n), dma(n), dma(2, n), dma(6, n), dma(n),
        reg(), reg(2), reg(2), reg(), reg(), reg(), reg(), reg(2), reg(), reg(),
    ]
    hbm = pl.BlockSpec(memory_space=pl.ANY)
    return pl.pallas_call(
        functools.partial(body, cfg),
        name="mlp_sums",
        out_shape=(jax.ShapeDtypeStruct((n, 2, 2, 4, 2, R, H), BF16), jax.ShapeDtypeStruct((n, 2, 4, 4, R, WB), BF16)),
        in_specs=[hbm] * 4,
        out_specs=(hbm, hbm),
        scratch_shapes=scratch,
        compiler_params=pltpu.CompilerParams(has_side_effects=True, vmem_limit_bytes=66_000_000),
    )(x, w_gate, w_up, w_down)


def place(cfg, ta, tb):
    n, R, D, WA, H, WB = (cfg[k] for k in ("n", "R", "D", "WA", "H", "WB"))
    W, NBUF = 8 * WA, 4

    def kernel(a_ref, b_ref, o_ref, buf, in_m, out_m):
        def ins(i, part, b):
            if part < 2:
                return [pltpu.make_async_copy(a_ref.at[i, part, o, g, k], buf.at[b, :, pl.ds((o * 4 + g) * WA + k * H, H)], in_m.at[b])
                        for o in range(2) for g in range(4) for k in range(2)]
            return [pltpu.make_async_copy(b_ref.at[i, c, q, g], buf.at[b, :, pl.ds(((c * 4 + q) * 4 + g) * WB, WB)], in_m.at[b])
                    for c in range(2) for q in range(4) for g in range(4)]

        def out(s, b):
            i, part = s // 3, s % 3
            rows = pl.ds(pl.multiple_of(i * R, R), R)
            return pltpu.make_async_copy(buf.at[b], o_ref.at[rows, pl.ds(pl.multiple_of(part * W, W), W)], out_m.at[b])

        def start(s):
            b = s % NBUF
            for part in range(3):
                @pl.when(s % 3 == part)
                def _():
                    for cp in ins(s // 3, part, b):
                        cp.start()

        for s in range(2):
            start(s)

        def step(s, _):
            @pl.when(s >= 2)
            def _():
                out(s - 2, (s - 2) % NBUF).wait()

            @pl.when(s + 2 < 3 * n)
            def _():
                start(s + 2)

            b = s % NBUF
            pltpu.make_async_copy(buf.at[b], buf.at[b], in_m.at[b]).wait()
            out(s, b).start()
            return 0

        lax.fori_loop(0, 3 * n, step, 0)
        for s in (3 * n - 2, 3 * n - 1):
            out(s, s % NBUF).wait()

    hbm = pl.BlockSpec(memory_space=pl.ANY)
    return pl.pallas_call(
        kernel,
        name="place",
        out_shape=jax.ShapeDtypeStruct((n * R, D), BF16),
        in_specs=[hbm, hbm],
        out_specs=hbm,
        scratch_shapes=[pltpu.VMEM((NBUF, R, W), BF16), pltpu.SemaphoreType.DMA((NBUF,)), pltpu.SemaphoreType.DMA((NBUF,))],
    )(ta, tb)


def build(mesh, chunk, pieces):
    def step(x, w_gate, w_up, w_down):
        cfg = dims(x.shape[0], x.shape[1], w_gate.shape[1], chunk, pieces)
        return place(cfg, *block_sums(cfg, x, w_gate, w_up, w_down))

    return jax.shard_map(
        step,
        mesh=mesh,
        in_specs=(P("dp", None), P(None, "tp"), P(None, "tp"), P("tp", None)),
        out_specs=P("dp", None),
        check_vma=False,
    )


def solution(mesh):
    return build(mesh, 256, 16)
```

```python
import functools

import jax
import jax.numpy as jnp
from jax import lax
from jax.experimental import pallas as pl
from jax.experimental.pallas import tpu as pltpu
from jax.sharding import PartitionSpec as P

F32 = jnp.float32
BF16 = jnp.bfloat16
MESH = pl.DeviceIdType.MESH


def dims(rows, d, ff, chunk, pieces):
    wa = d // 24
    return dict(n=rows // chunk, R=chunk, D=d, FF=ff, WA=wa, H=wa // 2, WB=wa // 4, NK=pieces, KB=d // pieces)


def body(cfg, x_ref, wg_ref, wu_ref, wdh_ref, ta, tb, wd, h, xb, wb, acc, ps, pr, a2s, a2r, a3s, a3r, t1s, t1r, t2s, t2r,
         b1s, b1r, b2s, b2r, b3s, b3r, b4s, b4r, b5s, b5r, fa, fb,
         wd_m, g_m, p_s, p_m, a2_s, a2_m, a3_s, a3_m, t1_s, t1_m, t2_s, t2_m, b1_s, b1_m, b2_s, b2_m, b3_s, b3_m, b4_s, b4_m, b5_s, b5_m,
         la_m, lb_m, fa_s, fb_s, q_s, g1_m, g2_m, g3_m, g4_m, g5_m, h1_m, h2_m, hz_m, h5_m,
         cp, ca2, ca3, ct1, ct2, cb1, cb2, cb3, cb4, cb5):
    n, R, D, FF, WA, H, WB, NK, KB = (cfg[k] for k in ("n", "R", "D", "FF", "WA", "H", "WB", "NK", "KB"))
    NB = xb.shape[0]
    me = lax.axis_index("tp")
    dp = lax.axis_index("dp")
    x, y, z, c = me // 16, (me // 8) % 2, (me // 2) % 4, me % 2

    def dev(x, y, z, c):
        return (dp, ((x * 2 + y) * 4 + z) * 2 + c)

    outer = (z == 0) | (z == 3)
    inner = jnp.logical_not(outer)
    up_ok, dn_ok = z < 3, z > 0
    zu, zd = jnp.minimum(z + 1, 3), jnp.maximum(z - 1, 0)
    zin = jnp.where(outer, jnp.where(z == 0, 1, 2), 3 - z)
    zout = jnp.where(z < 2, 0, 3)
    near = jnp.where(z < 2, 0, 1)
    far = 1 - near
    partner = dev(x, y, z, 1 - c)
    xn, yn = dev(1 - x, y, z, c), dev(x, 1 - y, z, c)
    up, down, zin_d, zout_d = dev(x, y, zu, c), dev(x, y, zd, c), dev(x, y, zin, c), dev(x, y, zout, c)
    go, gx, gy, gd = x * 2 + y, (1 - x) * 2 + y, x * 2 + 1 - y, (1 - x) * 2 + 1 - y

    def pick(order, a, b):
        first = order == 0
        return jax.tree.map(lambda p, q: jnp.where(first, p, q), a, b)

    def fn(order):
        return pick(order, xn, yn)

    def sn(order):
        return pick(order, yn, xn)

    def gf(order):
        return pick(order, gx, gy)

    def gs(order):
        return pick(order, gy, gx)

    def copy(src, dst, ss, rs, to):
        return pltpu.make_async_remote_copy(src, dst, ss, rs, device_id=to, device_id_type=MESH)

    def signal(sem, to):
        pl.semaphore_signal(sem, inc=1, device_id=to, device_id_type=MESH)

    def col_a(core, order, g, half=0):
        return core * (8 * WA) + order * (4 * WA) + g * WA + half * H

    def col_b(core, q, g=0):
        return 16 * WA + core * (16 * WB) + q * (4 * WB) + g * WB

    def lanes(i, w):
        return pl.ds(pl.multiple_of(i * w, w), w)

    def dot(i, col, w, unit):
        return jnp.dot(h[i % 3], wd[:, pl.ds(pl.multiple_of(col, unit), w)], preferred_element_type=F32)

    def c_p(s):
        return copy(ps, pr.at[s], p_s, p_m.at[s], partner)

    def c_a2(s, o, m):
        return copy(a2s.at[o, m], a2r.at[s, o, m], a2_s.at[o, m], a2_m.at[s, o, m], fn(o))

    def c_a3(s, o):
        return copy(a3s.at[o], a3r.at[s, o], a3_s.at[o], a3_m.at[s, o], sn(o))

    def c_t1(o):
        return copy(t1s.at[o], t1r.at[o], t1_s.at[o], t1_m.at[o], zin_d)

    def c_t2(src, o):
        return copy(t2s.at[o], t2r.at[src, o], t2_s.at[o], t2_m.at[src, o], zin_d)

    def c_b1():
        return copy(b1s, b1r, b1_s, b1_m, zin_d)

    def c_b2(d):
        return copy(b2s, b2r.at[d], b2_s, b2_m.at[d], zin_d)

    def c_b3(d, to=up):
        return copy(b3s.at[d], b3r.at[d], b3_s.at[d], b3_m.at[d], to)

    def c_b4(o, m):
        return copy(b4s.at[m], b4r.at[m], b4_s.at[m], b4_m.at[m], fn(o))

    def c_b5(o):
        return copy(b5s, b5r, b5_s, b5_m, sn(o))

    def g_copies(kk):
        i, k, b = kk // NK, kk % NK, kk % NB
        rows, ks = pl.ds(pl.multiple_of(i * R, R), R), pl.ds(pl.multiple_of(k * KB, KB), KB)
        return (pltpu.make_async_copy(x_ref.at[rows, ks], xb.at[b], g_m.at[b, 0]),
                pltpu.make_async_copy(wg_ref.at[ks], wb.at[b, :, pl.ds(0, FF)], g_m.at[b, 1]),
                pltpu.make_async_copy(wu_ref.at[ks], wb.at[b, :, pl.ds(FF, FF)], g_m.at[b, 2]))

    def wd_copy(k):
        core, m = jnp.where(k < 3, 1 - c, c), k % 3
        off = jnp.where(m < 2, col_a(core, m, 0), col_b(core, 0))
        cols = pl.ds(pl.multiple_of(off, 4 * WA), 4 * WA)
        return pltpu.make_async_copy(wdh_ref.at[:, cols], wd.at[:, cols], wd_m.at[k])

    def g_pieces(i, k0, k1):
        def step(k, _):
            kk = i * NK + k
            b = kk % NB
            for cp_ in g_copies(kk):
                cp_.wait()

            @pl.when(kk == NK - 1)
            def _():
                for p in range(6):
                    wd_copy(p).start()

            @pl.when((kk + NB - 1 < n * NK))
            def _():
                for cp_ in g_copies(kk + NB - 1):
                    cp_.start()

            @pl.when(k == 0)
            def _():
                acc[...] = jnp.zeros_like(acc)

            acc[...] += jnp.dot(xb[b], wb[b], preferred_element_type=F32)
            return 0

        lax.fori_loop(k0, k1, step, 0)
        if k1 == NK:
            h[i % 3] = (jax.nn.silu(acc[:, :FF]) * acc[:, FF:]).astype(BF16)

    def s1(t):
        @pl.when(t >= 1)
        def _():
            c_p(0).wait_send()

        @pl.when(t >= 2)
        def _():
            pl.semaphore_wait(cp, 1)

        def step(j, _):
            @pl.when((t == 0) & (j % 4 == 0))
            def _():
                wd_copy(j // 4).wait()

            col = jnp.where(j < 8, col_a(1 - c, 0, j), col_b(1 - c, j - 8))
            ps[j] = dot(t, col, WA, WA).astype(BF16)
            copy(ps.at[j], pr.at[t % 2, j], p_s, p_m.at[t % 2], partner).start()
            return 0

        lax.fori_loop(0, 12, step, 0)

    def s2(t, m):
        def step(o, _):
            @pl.when(t >= 1)
            def _():
                c_a2(0, o, m).wait_send()

            if m == 0:
                @pl.when(t >= 2)
                def _():
                    pl.semaphore_wait(ca2.at[o], 1)

            g = gf(o) if m else gd
            v = dot(t, col_a(c, o, g), WA, WA) + pr[t % 2, o * 4 + g].astype(F32)
            a2s[o, m] = v.astype(BF16)
            c_a2(t % 2, o, m).start()
            return 0

        lax.fori_loop(0, 2, step, 0)

    def s3(t):
        def step(o, _):
            @pl.when(t >= 1)
            def _():
                c_a3(0, o).wait_send()

            @pl.when(t >= 2)
            def _():
                pl.semaphore_wait(ca3.at[o], 1)

            c_a2(t % 2, o, 0).wait_recv()
            g = gs(o)
            v = dot(t, col_a(c, o, g), WA, WA) + pr[t % 2, o * 4 + g].astype(F32) + a2r[t % 2, o, 0].astype(F32)
            a3s[o] = v.astype(BF16)
            c_a3(t % 2, o).start()
            return 0

        lax.fori_loop(0, 2, step, 0)

    def t1(t):
        @pl.when(t == 0)
        def _():
            for p in range(3, 6):
                wd_copy(p).wait()

        c_p(t % 2).wait_recv()

        @pl.when(outer)
        def _():
            @pl.when(t >= 1)
            def _():
                c_b1().wait_send()
                pl.semaphore_wait(cb1, 1)

            q = 3 - z
            b1s[...] = (dot(t, col_b(c, q), WA, WA) + pr[t % 2, 8 + q].astype(F32)).astype(BF16)
            c_b1().start()

    def t2(t):
        @pl.when(t >= 1)
        def _():
            c_b2(0).wait_send()
            pl.semaphore_wait(cb2, 1)

        @pl.when(inner)
        def _():
            c_b1().wait_recv()

        q = (z + 2) % 4
        b2s[...] = (dot(t, col_b(c, q), WA, WA) + pr[t % 2, 8 + q].astype(F32) + b1r[...].astype(F32)).astype(BF16)
        d = jnp.where(z < 2, 0, 1)
        c_b2(d).start()

        @pl.when(inner & (t + 1 < n))
        def _():
            signal(cb1, zout_d)

    def s4(u):
        for o in range(2):
            c_a3(u % 2, o).wait_recv()
            c_a2(u % 2, o, 1).wait_recv()

        @pl.when(outer)
        def _():
            def step(o, _):
                @pl.when(u >= 1)
                def _():
                    c_t1(o).wait_send()

                @pl.when((u >= 1) & (o == 0))
                def _():
                    pl.semaphore_wait(ct1, 1)

                t1s[o] = own_a(u, o, far).astype(BF16)
                c_t1(o).start()
                return 0

            lax.fori_loop(0, 2, step, 0)

    def own_a(u, o, half):
        s, ln = u % 2, lanes(half, H)
        return (dot(u, col_a(c, o, go, half), H, H) + pr[s, o * 4 + go, :, ln].astype(F32)
                + a2r[s, o, 1, :, ln].astype(F32) + a3r[s, o, :, ln].astype(F32))

    def s5(u):
        src = jnp.where(outer, 0, 1)

        def step(o, _):
            @pl.when(u >= 1)
            def _():
                c_t2(src, o).wait_send()

            @pl.when((u >= 1) & (o == 0))
            def _():
                pl.semaphore_wait(ct2, 1)

            @pl.when(inner)
            def _():
                c_t1(o).wait_recv()

            half = jnp.where(outer, near, far)
            t2s[o] = (own_a(u, o, half) + t1r[o].astype(F32)).astype(BF16)
            c_t2(src, o).start()
            return 0

        lax.fori_loop(0, 2, step, 0)

        @pl.when(inner & (u + 1 < n))
        def _():
            signal(ct1, zout_d)

    def win_a(u, o, g, half):
        return ta.at[u, c, o, g, half]

    def fa_copies(u, o):
        w = win_a(u, o, go, near)
        f = fa.at[o]
        return ((f, w, fa_s.at[o, 0], g1_m.at[u], zout_d), (f, w, fa_s.at[o, 1], g1_m.at[u], zin_d),
                (f, w, fa_s.at[o, 2], g3_m.at[0, u], sn(o)), (f, w, fa_s.at[o, 3], g4_m.at[0, u], fn(o)),
                (f, w, fa_s.at[o, 4], g5_m.at[u], partner))

    def fa_done(u, o):
        for a in fa_copies(u, o):
            copy(*a).wait_send()
        pltpu.make_async_copy(fa.at[o], win_a(u, o, go, near), la_m.at[o]).wait()

    def s6(u):
        @pl.when(inner)
        def _():
            for o in range(2):
                for src in range(2):
                    c_t2(src, o).wait_recv()

            def step(o, _):
                @pl.when(u >= 1)
                def _():
                    fa_done(u, o)

                fa[o] = (own_a(u, o, near) + t2r[0, o].astype(F32) + t2r[1, o].astype(F32)).astype(BF16)
                pltpu.make_async_copy(fa.at[o], win_a(u, o, go, near), la_m.at[o]).start()
                for a in fa_copies(u, o):
                    copy(*a).start()
                return 0

            lax.fori_loop(0, 2, step, 0)

            @pl.when(u + 1 < n)
            def _():
                signal(ct2, zout_d)
                signal(ct2, zin_d)

        @pl.when(u + 2 < n)
        def _():
            for o in range(2):
                signal(ca2.at[o], fn(o))
                signal(ca3.at[o], sn(o))

    def t3(u):
        def step(d, _):
            ok = jnp.where(d == 0, up_ok, dn_ok)

            @pl.when(ok)
            def _():
                to = pick(d, up, down)

                @pl.when(u >= 1)
                def _():
                    c_b3(d, to).wait_send()
                    pl.semaphore_wait(cb3.at[d], 1)

                @pl.when(inner)
                def _():
                    c_b2(d).wait_recv()

                q = pick(d, zu, zd)
                b3s[d] = (dot(u, col_b(c, q), WA, WA) + pr[u % 2, 8 + q].astype(F32) + b2r[d].astype(F32)).astype(BF16)
                c_b3(d, to).start()

            return 0

        lax.fori_loop(0, 2, step, 0)

        @pl.when(inner & (u + 1 < n))
        def _():
            signal(cb2, zout_d)
            signal(cb2, zin_d)

    def own_b(u, g):
        ln = lanes(g, WB)
        return (dot(u, col_b(c, z, g), WB, WB) + pr[u % 2, 8 + z, :, ln].astype(F32)
                + b3r[0, :, ln].astype(F32) + b3r[1, :, ln].astype(F32))

    def t4(u):
        @pl.when(dn_ok)
        def _():
            c_b3(0).wait_recv()

        @pl.when(up_ok)
        def _():
            c_b3(1).wait_recv()

        o = u % 2

        def step(m, _):
            @pl.when(u >= 1)
            def _():
                c_b4(o, m).wait_send()

            @pl.when((u >= 1) & (m == 0))
            def _():
                pl.semaphore_wait(cb4, 1)

            b4s[m] = own_b(u, jnp.where(m == 0, gd, gf(o))).astype(BF16)
            c_b4(o, m).start()
            return 0

        lax.fori_loop(0, 2, step, 0)

    def t5(u):
        o = u % 2

        @pl.when(u >= 1)
        def _():
            c_b5(o).wait_send()
            pl.semaphore_wait(cb5, 1)

        c_b4(o, 0).wait_recv()
        b5s[...] = (own_b(u, gs(o)) + b4r[0].astype(F32)).astype(BF16)
        c_b5(o).start()

    def fb_copies(u):
        w, o = tb.at[u, c, z, go], u % 2
        return ((fb, w, fb_s.at[0], h1_m.at[u], sn(o)), (fb, w, fb_s.at[1], h2_m.at[0, u], fn(o)))

    def fb_local(u):
        return pltpu.make_async_copy(fb, tb.at[u, c, z, go], lb_m)

    def t6(u):
        o = u % 2
        c_b4(o, 1).wait_recv()
        c_b5(o).wait_recv()

        @pl.when(u >= 1)
        def _():
            for a in fb_copies(u):
                copy(*a).wait_send()

        fb[...] = (own_b(u, go) + b4r[1].astype(F32) + b5r[...].astype(F32)).astype(BF16)
        fb_local(u).start()
        for a in fb_copies(u):
            copy(*a).start()

        @pl.when(u + 1 < n)
        def _():
            @pl.when(dn_ok)
            def _():
                signal(cb3.at[0], down)

            @pl.when(up_ok)
            def _():
                signal(cb3.at[1], up)

            signal(cb4, fn(1 - o))
            signal(cb5, sn(1 - o))

        @pl.when(u + 2 < n)
        def _():
            signal(cp, partner)

    def go_on(v, cond, k, src, rs, to):
        def make():
            return copy(src(v), src(v), q_s.at[k], rs(v), to)

        @pl.when(cond if cond is not True else v >= 0)
        def _():
            @pl.when(v >= 1)
            def _():
                make().wait_send()

            make().start()

    plan = []

    def op(group, cond, src, rs, to):
        plan.append((group, cond, len(plan), src, rs, to))

    def half_ops(group, cond, half, which):
        for o in range(2):
            w = functools.partial(lambda o, half, v: win_a(v, o, go, half), o, half)
            op(group, cond, w, functools.partial(lambda k, v: g3_m.at[k, v], which), sn(o))
            op(group, cond, w, functools.partial(lambda k, v: g4_m.at[k, v], which), fn(o))
            op(group, cond, w, lambda v: g5_m.at[v], partner)

    for o in range(2):
        op("q0", inner, functools.partial(lambda o, v: win_a(v, o, go, far), o), lambda v: g2_m.at[v], zout_d)
    half_ops("q0i", inner, far, 1)
    half_ops("q0o", outer, near, 0)
    half_ops("q1", outer, far, 1)
    for k, half in ((0, near), (1, far)):
        for o in range(2):
            w = functools.partial(lambda o, half, v: win_a(v, o, gs(o), half), o, half)
            op(f"q{2 + k}", True, w, functools.partial(lambda k, v: g4_m.at[2 + k, v], k), fn(o))
            op(f"q{2 + k}", True, w, lambda v: g5_m.at[v], partner)
    for o in range(2):
        for half in range(2):
            op("q4", True, functools.partial(lambda o, half, v: win_a(v, o, gf(o), half), o, half), lambda v: g5_m.at[v], partner)
            op("q5", True, functools.partial(lambda o, half, v: win_a(v, o, gd, half), o, half), lambda v: g5_m.at[v], partner)
    op("r0", True, lambda v: tb.at[v, c, z, gs(v % 2)], lambda v: h2_m.at[1, v], None)
    block = lambda q: (lambda v: tb.at[v, c, q])
    op("r1", up_ok, block(z), lambda v: hz_m.at[0, v], up)
    op("r1", dn_ok, block(z), lambda v: hz_m.at[1, v], down)
    op("r1", True, block(z), lambda v: h5_m.at[v], partner)
    zm2, zp2 = jnp.maximum(z - 2, 0), jnp.minimum(z + 2, 3)
    op("r2u", dn_ok & up_ok, block(zd), lambda v: hz_m.at[2, v], up)
    op("r2u", dn_ok, block(zd), lambda v: h5_m.at[v], partner)
    op("r2d", dn_ok & up_ok, block(zu), lambda v: hz_m.at[3, v], down)
    op("r2d", up_ok, block(zu), lambda v: h5_m.at[v], partner)
    op("r3u", z == 2, block(zm2), lambda v: hz_m.at[4, v], up)
    op("r3u", z >= 2, block(zm2), lambda v: h5_m.at[v], partner)
    op("r3d", z == 1, block(zp2), lambda v: hz_m.at[5, v], down)
    op("r3d", z <= 1, block(zp2), lambda v: h5_m.at[v], partner)
    op("r4", outer, block(3 - z), lambda v: h5_m.at[v], partner)

    def run(group, v):
        for g_, cond, k, src, rs, to in plan:
            if g_ == group:
                go_on(v, cond, k, src, rs, fn(v % 2) if to is None else to)

    def arrived(ref, sem):
        copy(ref, ref, q_s.at[0], sem, partner).wait_recv()

    def pair(v):
        return ta.at[v, c, :, 0, 0]

    def q0a(v):
        arrived(pair(v), g1_m.at[v])
        run("q0", v)
        run("q0i", v)
        run("q0o", v)

    def q0b(v):
        arrived(tb.at[v, c, 0, 0], h1_m.at[v])
        run("r0", v)

    def q1a(v):
        @pl.when(outer)
        def _():
            arrived(pair(v), g2_m.at[v])

        run("q1", v)

    def q1b(v):
        fb_local(v).wait()
        for k in range(2):
            arrived(tb.at[v, c, 0, 0], h2_m.at[k, v])
        run("r1", v)

    def q2a(v):
        arrived(pair(v), g3_m.at[0, v])
        run("q2", v)

    def q3a(v):
        arrived(pair(v), g3_m.at[1, v])
        run("q3", v)

    def hop(v, up_there, down_there, k, groups):
        for there, kk, g in ((up_there, k, groups[0]), (down_there, k + 1, groups[1])):
            @pl.when(there)
            def _():
                arrived(tb.at[v, c, 0], hz_m.at[kk, v])

            run(g, v)

    def q2b(v):
        hop(v, dn_ok, up_ok, 0, ("r2u", "r2d"))

    def q3b(v):
        hop(v, z >= 2, z <= 1, 2, ("r3u", "r3d"))

    def q4b(v):
        hop(v, z == 3, z == 0, 4, ("", "r4"))

    def q4a(v):
        for k in range(2):
            arrived(pair(v), g4_m.at[k, v])
        run("q4", v)

    def q5(v):
        for k in range(2):
            arrived(pair(v), g4_m.at[2 + k, v])
        run("q5", v)

    @pl.when(outer)
    def _():
        t1r[...] = jnp.zeros_like(t1r)
        b1r[...] = jnp.zeros_like(b1r)
        b2r[...] = jnp.zeros_like(b2r)

    @pl.when(z == 0)
    def _():
        b3r[0] = jnp.zeros_like(b3r[0])

    @pl.when(z == 3)
    def _():
        b3r[1] = jnp.zeros_like(b3r[1])

    for kk in range(NB - 1):
        for cp_ in g_copies(kk):
            cp_.start()

    g_pieces(0, 0, NK)
    s1(0)
    cut = [NK * k // 8 for k in range(9)]

    def slot(t, _):
        def at(i, f):
            @pl.when((i >= 0) & (i < n))
            def _():
                f(i)

        def g(a, b):
            at(t + 1, lambda i: g_pieces(i, cut[a], cut[b]))

        u, v, w, e = t - 1, t - 2, t - 3, t - 4
        at(v, q0a)
        at(t - 8, q4b)
        at(u, s4)
        g(0, 1)
        at(t, t1)
        at(u, t4)
        at(t, lambda i: s2(i, 0))
        at(u, s5)
        at(v, q1b)
        at(t - 7, q4a)
        g(1, 2)
        at(u, t5)
        at(t - 7, q3a)
        at(t, lambda i: s2(i, 1))
        g(2, 3)
        at(e, q2a)
        at(e, q3b)
        g(3, 4)
        at(t, t2)
        g(4, 6)
        at(u, s6)
        at(u, t6)
        at(t, s3)
        g(6, 8)
        at(v, q1a)
        at(t - 8, q5)
        at(t, t3)
        at(v, q2b)
        at(t + 1, s1)
        at(u, q0b)
        return 0

    lax.fori_loop(0, n + 8, slot, 0)

    last = n - 1
    c_p(0).wait_send()
    for o in range(2):
        for m in range(2):
            c_a2(0, o, m).wait_send()
        c_b4(0, o).wait_send()
        c_a3(0, o).wait_send()
        c_t2(0, o).wait_send()

        @pl.when(outer)
        def _():
            c_t1(o).wait_send()

        @pl.when(inner)
        def _():
            fa_done(last, o)

        @pl.when(up_ok if o == 0 else dn_ok)
        def _():
            c_b3(o).wait_send()

    @pl.when(outer)
    def _():
        c_b1().wait_send()

    c_b2(0).wait_send()
    c_b5(0).wait_send()
    for a in fb_copies(last):
        copy(*a).wait_send()
    for g_, cond, k, src, rs, to in plan:
        def done(k=k, src=src, rs=rs):
            copy(src(last), src(last), q_s.at[k], rs(last), partner).wait_send()

        if cond is True:
            done()
        else:
            pl.when(cond)(done)

    def all_here(v, _):
        arrived(ta.at[v, 1 - c], g5_m.at[v])
        arrived(tb.at[v, 1 - c], h5_m.at[v])
        return 0

    lax.fori_loop(0, n, all_here, 0)


N_OPS = 2 + 6 * 3 + 8 + 8 + 1 + 3 + 8 + 1


def block_sums(cfg, x, w_gate, w_up, w_down):
    n, R, D, FF, WA, H, WB, KB = (cfg[k] for k in ("n", "R", "D", "FF", "WA", "H", "WB", "KB"))
    NB = 3
    vm = lambda *s: pltpu.VMEM(s, BF16)
    dma = lambda *s: pltpu.SemaphoreType.DMA(s) if s else pltpu.SemaphoreType.DMA
    reg = lambda *s: pltpu.SemaphoreType.REGULAR(s) if s else pltpu.SemaphoreType.REGULAR
    scratch = [
        vm(FF, D), vm(3, R, FF), vm(NB, R, KB), vm(NB, KB, 2 * FF), pltpu.VMEM((R, 2 * FF), F32),
        vm(12, R, WA), vm(2, 12, R, WA), vm(2, 2, R, WA), vm(2, 2, 2, R, WA), vm(2, R, WA), vm(2, 2, R, WA),
        vm(2, R, H), vm(2, R, H), vm(2, R, H), vm(2, 2, R, H),
        vm(R, WA), vm(R, WA), vm(R, WA), vm(2, R, WA), vm(2, R, WA), vm(2, R, WA), vm(2, R, WB), vm(2, R, WB), vm(R, WB), vm(R, WB),
        vm(2, R, H), vm(R, WB),
        dma(6), dma(NB, 3), dma(), dma(2), dma(2, 2), dma(2, 2, 2), dma(2), dma(2, 2), dma(2), dma(2), dma(2), dma(2, 2),
        dma(), dma(), dma(), dma(2), dma(2), dma(2), dma(2), dma(2), dma(), dma(),
        dma(2), dma(), dma(2, 5), dma(2), dma(N_OPS), dma(n), dma(n), dma(2, n), dma(4, n), dma(n), dma(n), dma(2, n), dma(6, n), dma(n),
        reg(), reg(2), reg(2), reg(), reg(), reg(), reg(), reg(2), reg(), reg(),
    ]
    hbm = pl.BlockSpec(memory_space=pl.ANY)
    return pl.pallas_call(
        functools.partial(body, cfg),
        name="mlp_sums",
        out_shape=(jax.ShapeDtypeStruct((n, 2, 2, 4, 2, R, H), BF16), jax.ShapeDtypeStruct((n, 2, 4, 4, R, WB), BF16)),
        in_specs=[hbm] * 4,
        out_specs=(hbm, hbm),
        scratch_shapes=scratch,
        compiler_params=pltpu.CompilerParams(has_side_effects=True, vmem_limit_bytes=66_000_000),
    )(x, w_gate, w_up, w_down)


def place(cfg, ta, tb):
    n, R, D, WA, H, WB = (cfg[k] for k in ("n", "R", "D", "WA", "H", "WB"))
    W, NBUF, AHEAD = 8 * WA, 8, 4

    def kernel(a_ref, b_ref, o_ref, buf, in_m, out_m):
        def ins(i, part, b):
            if part < 2:
                return [pltpu.make_async_copy(a_ref.at[i, part, o, g, k], buf.at[b, :, pl.ds((o * 4 + g) * WA + k * H, H)], in_m.at[b])
                        for o in range(2) for g in range(4) for k in range(2)]
            return [pltpu.make_async_copy(b_ref.at[i, c, q, g], buf.at[b, :, pl.ds(((c * 4 + q) * 4 + g) * WB, WB)], in_m.at[b])
                    for c in range(2) for q in range(4) for g in range(4)]

        def out(s, b):
            i, part = s // 3, s % 3
            rows = pl.ds(pl.multiple_of(i * R, R), R)
            return pltpu.make_async_copy(buf.at[b], o_ref.at[rows, pl.ds(pl.multiple_of(part * W, W), W)], out_m.at[b])

        def start(s):
            b = s % NBUF
            for part in range(3):
                @pl.when(s % 3 == part)
                def _():
                    for cp in ins(s // 3, part, b):
                        cp.start()

        for s in range(AHEAD):
            start(s)

        def step(s, _):
            @pl.when(s >= NBUF - AHEAD)
            def _():
                out(s - NBUF + AHEAD, (s + AHEAD) % NBUF).wait()

            @pl.when(s + AHEAD < 3 * n)
            def _():
                start(s + AHEAD)

            b = s % NBUF
            pltpu.make_async_copy(buf.at[b], buf.at[b], in_m.at[b]).wait()
            out(s, b).start()
            return 0

        lax.fori_loop(0, 3 * n, step, 0)
        for s in range(3 * n - NBUF + AHEAD, 3 * n):
            out(s, s % NBUF).wait()

    hbm = pl.BlockSpec(memory_space=pl.ANY)
    return pl.pallas_call(
        kernel,
        name="place",
        out_shape=jax.ShapeDtypeStruct((n * R, D), BF16),
        in_specs=[hbm, hbm],
        out_specs=hbm,
        scratch_shapes=[pltpu.VMEM((NBUF, R, W), BF16), pltpu.SemaphoreType.DMA((NBUF,)), pltpu.SemaphoreType.DMA((NBUF,))],
    )(ta, tb)


def build(mesh, chunk, pieces):
    def step(x, w_gate, w_up, w_down):
        cfg = dims(x.shape[0], x.shape[1], w_gate.shape[1], chunk, pieces)
        return place(cfg, *block_sums(cfg, x, w_gate, w_up, w_down))

    return jax.shard_map(
        step,
        mesh=mesh,
        in_specs=(P("dp", None), P(None, "tp"), P(None, "tp"), P("tp", None)),
        out_specs=P("dp", None),
        check_vma=False,
    )


def solution(mesh):
    return build(mesh, 256, 12)
```

```python
import functools
import math

import jax
import jax.numpy as jnp
from jax import lax
from jax.experimental import pallas as pl
from jax.experimental.pallas import tpu as pltpu
from jax.sharding import PartitionSpec as P

F32 = jnp.float32
BF16 = jnp.bfloat16
MESH = pl.DeviceIdType.MESH


def dims(rows, d, ff, chunk, pieces):
    wa = d // 24
    return dict(n=rows // chunk, R=chunk, D=d, FF=ff, WA=wa, H=wa // 2, WB=wa // 4, NK=pieces, KB=d // pieces)


def staged(cfg):
    return min((cfg["FF"] + cfg["KB"]) // cfg["R"], cfg["n"] - 1)


def body(cfg, x_ref, wg_ref, wu_ref, wdh_ref, tot, big, h, xb, acc, a2s, a2r, a3s, a3r, t1s, t1r, t2s, t2r,
         b1s, b1r, b2s, b2r, b3s, b3r, b4s, b4r, b5s, b5r, fa, fb,
         wd_m, g_m, st_m, p_s, p_m, a2_s, a2_m, a3_s, a3_m, t1_s, t1_m, t2_s, t2_m, b1_s, b1_m, b2_s, b2_m, b3_s, b3_m, b4_s, b4_m, b5_s, b5_m,
         la_m, lb_m, fa_s, fb_s, q_s, g1_m, g2_m, g3_m, g4_m, g5_m, h1_m, h2_m, hz_m, h5_m,
         cp, ca2, ca3, ct1, ct2, cb1, cb2, cb3, cb4, cb5):
    n, R, D, FF, WA, H, WB, NK, KB = (cfg[k] for k in ("n", "R", "D", "FF", "WA", "H", "WB", "NK", "KB"))
    NB = xb.shape[0]
    S = staged(cfg)
    me = lax.axis_index("tp")
    dp = lax.axis_index("dp")
    x, y, z, c = me // 16, (me // 8) % 2, (me // 2) % 4, me % 2

    def dev(x, y, z, c):
        return (dp, ((x * 2 + y) * 4 + z) * 2 + c)

    outer = (z == 0) | (z == 3)
    inner = jnp.logical_not(outer)
    up_ok, dn_ok = z < 3, z > 0
    zu, zd = jnp.minimum(z + 1, 3), jnp.maximum(z - 1, 0)
    zin = jnp.where(outer, jnp.where(z == 0, 1, 2), 3 - z)
    zout = jnp.where(z < 2, 0, 3)
    near = jnp.where(z < 2, 0, 1)
    far = 1 - near
    partner = dev(x, y, z, 1 - c)
    xn, yn = dev(1 - x, y, z, c), dev(x, 1 - y, z, c)
    up, down, zin_d, zout_d = dev(x, y, zu, c), dev(x, y, zd, c), dev(x, y, zin, c), dev(x, y, zout, c)
    go, gx, gy, gd = x * 2 + y, (1 - x) * 2 + y, x * 2 + 1 - y, (1 - x) * 2 + 1 - y

    def pick(order, a, b):
        first = order == 0
        return jax.tree.map(lambda p, q: jnp.where(first, p, q), a, b)

    def fn(order):
        return pick(order, xn, yn)

    def sn(order):
        return pick(order, yn, xn)

    def gf(order):
        return pick(order, gx, gy)

    def gs(order):
        return pick(order, gy, gx)

    def copy(src, dst, ss, rs, to):
        return pltpu.make_async_remote_copy(src, dst, ss, rs, device_id=to, device_id_type=MESH)

    def signal(sem, to):
        pl.semaphore_signal(sem, inc=1, device_id=to, device_id_type=MESH)

    def col_a(core, order, g, half=0):
        return core * (8 * WA) + order * (4 * WA) + g * WA + half * H

    def col_b(core, q, g=0):
        return 16 * WA + core * (16 * WB) + q * (4 * WB) + g * WB

    def lanes(i, w):
        return pl.ds(pl.multiple_of(i * w, w), w)

    def dot(i, col, w, unit):
        return jnp.dot(h[i % 3], big[pl.ds(0, FF), pl.ds(pl.multiple_of(col, unit), w)], preferred_element_type=F32)

    def weights(b, off, w):
        return pl.ds(FF, KB), pl.ds(pl.multiple_of(b * 2 * FF + off, FF), w)

    def tile(k, off=0, w=WA):
        across, first = (D - NB * 2 * FF) // WA, NB * 2 * FF
        row, col = FF + k // across * R, first + k % across * WA + off
        return (pl.ds(pl.multiple_of(row, math.gcd(FF, R)), R), pl.ds(pl.multiple_of(col, math.gcd(first, WB)), w))

    def p_in(s, j, off=0, w=WA):
        return big[tile(s * 12 + j, off, w)].astype(F32)

    def p_tile(k):
        return big.at[tile(k)]

    def c_p(s):
        every = big.at[pl.ds(0, R), pl.ds(0, 12 * WA)]
        return copy(every, every, p_s, p_m.at[s], partner)

    def c_a2(s, o, m):
        return copy(a2s.at[o, m], a2r.at[s, o, m], a2_s.at[o, m], a2_m.at[s, o, m], fn(o))

    def c_a3(s, o):
        return copy(a3s.at[o], a3r.at[s, o], a3_s.at[o], a3_m.at[s, o], sn(o))

    def c_t1(o):
        return copy(t1s.at[o], t1r.at[o], t1_s.at[o], t1_m.at[o], zin_d)

    def c_t2(src, o):
        return copy(t2s.at[o], t2r.at[src, o], t2_s.at[o], t2_m.at[src, o], zin_d)

    def c_b1():
        return copy(b1s, b1r, b1_s, b1_m, zin_d)

    def c_b2(d):
        return copy(b2s, b2r.at[d], b2_s, b2_m.at[d], zin_d)

    def c_b3(d, to=up):
        return copy(b3s.at[d], b3r.at[d], b3_s.at[d], b3_m.at[d], to)

    def c_b4(o, m):
        return copy(b4s.at[m], b4r.at[m], b4_s.at[m], b4_m.at[m], fn(o))

    def c_b5(o):
        return copy(b5s, b5r, b5_s, b5_m, sn(o))

    def g_copies(kk):
        i, k, b = kk // NK, kk % NK, kk % NB
        rows, ks = pl.ds(pl.multiple_of(i * R, R), R), pl.ds(pl.multiple_of(k * KB, KB), KB)
        return (pltpu.make_async_copy(x_ref.at[rows, ks], xb.at[b], g_m.at[b, 0]),
                pltpu.make_async_copy(wg_ref.at[ks], big.at[weights(b, 0, FF)], g_m.at[b, 1]),
                pltpu.make_async_copy(wu_ref.at[ks], big.at[weights(b, FF, FF)], g_m.at[b, 2]))

    def wd_copy(k):
        core, m = jnp.where(k < 3, 1 - c, c), k % 3
        off = jnp.where(m < 2, col_a(core, m, 0), col_b(core, 0))
        cols = pl.ds(pl.multiple_of(off, 4 * WA), 4 * WA)
        return pltpu.make_async_copy(wdh_ref.at[:, cols], big.at[pl.ds(0, FF), cols], wd_m.at[k])

    def g_pieces(i, k0, k1):
        def step(k, _):
            kk = i * NK + k
            b = kk % NB
            for cp_ in g_copies(kk):
                cp_.wait()

            @pl.when(kk == NK - 1)
            def _():
                for p in range(6):
                    wd_copy(p).start()

            @pl.when((kk + NB - 1 < n * NK))
            def _():
                for cp_ in g_copies(kk + NB - 1):
                    cp_.start()

            @pl.when(k == 0)
            def _():
                acc[...] = jnp.zeros_like(acc)

            acc[...] += jnp.dot(xb[b], big[weights(b, 0, 2 * FF)], preferred_element_type=F32)
            return 0

        lax.fori_loop(k0, k1, step, 0)
        if k1 == NK:
            h[i % 3] = (jax.nn.silu(acc[:, :FF]) * acc[:, FF:]).astype(BF16)

    def s1(t):
        @pl.when(t >= 1)
        def _():
            c_p(0).wait_send()

        @pl.when(t >= 2)
        def _():
            pl.semaphore_wait(cp, 1)

        def step(j, _):
            @pl.when((t == 0) & (j % 4 == 0))
            def _():
                wd_copy(j // 4).wait()

            col = jnp.where(j < 8, col_a(1 - c, 0, j), col_b(1 - c, j - 8))
            p_tile(24 + j)[...] = dot(t, col, WA, WA).astype(BF16)
            copy(p_tile(24 + j), p_tile(t % 2 * 12 + j), p_s, p_m.at[t % 2], partner).start()
            return 0

        lax.fori_loop(0, 12, step, 0)

    def s2(t, m):
        def step(o, _):
            @pl.when(t >= 1)
            def _():
                c_a2(0, o, m).wait_send()

            if m == 0:
                @pl.when(t >= 2)
                def _():
                    pl.semaphore_wait(ca2.at[o], 1)

            g = gf(o) if m else gd
            v = dot(t, col_a(c, o, g), WA, WA) + p_in(t % 2, o * 4 + g)
            a2s[o, m] = v.astype(BF16)
            c_a2(t % 2, o, m).start()
            return 0

        lax.fori_loop(0, 2, step, 0)

    def s3(t):
        def step(o, _):
            @pl.when(t >= 1)
            def _():
                c_a3(0, o).wait_send()

            @pl.when(t >= 2)
            def _():
                pl.semaphore_wait(ca3.at[o], 1)

            c_a2(t % 2, o, 0).wait_recv()
            g = gs(o)
            v = dot(t, col_a(c, o, g), WA, WA) + p_in(t % 2, o * 4 + g) + a2r[t % 2, o, 0].astype(F32)
            a3s[o] = v.astype(BF16)
            c_a3(t % 2, o).start()
            return 0

        lax.fori_loop(0, 2, step, 0)

    def t1(t):
        @pl.when(t == 0)
        def _():
            for p in range(3, 6):
                wd_copy(p).wait()

        c_p(t % 2).wait_recv()

        @pl.when(outer)
        def _():
            @pl.when(t >= 1)
            def _():
                c_b1().wait_send()
                pl.semaphore_wait(cb1, 1)

            q = 3 - z
            b1s[...] = (dot(t, col_b(c, q), WA, WA) + p_in(t % 2, 8 + q)).astype(BF16)
            c_b1().start()

    def t2(t):
        @pl.when(t >= 1)
        def _():
            c_b2(0).wait_send()
            pl.semaphore_wait(cb2, 1)

        @pl.when(inner)
        def _():
            c_b1().wait_recv()

        q = (z + 2) % 4
        b2s[...] = (dot(t, col_b(c, q), WA, WA) + p_in(t % 2, 8 + q) + b1r[...].astype(F32)).astype(BF16)
        d = jnp.where(z < 2, 0, 1)
        c_b2(d).start()

        @pl.when(inner & (t + 1 < n))
        def _():
            signal(cb1, zout_d)

    def s4(u):
        for o in range(2):
            c_a3(u % 2, o).wait_recv()
            c_a2(u % 2, o, 1).wait_recv()

        @pl.when(outer)
        def _():
            def step(o, _):
                @pl.when(u >= 1)
                def _():
                    c_t1(o).wait_send()

                @pl.when((u >= 1) & (o == 0))
                def _():
                    pl.semaphore_wait(ct1, 1)

                t1s[o] = own_a(u, o, far).astype(BF16)
                c_t1(o).start()
                return 0

            lax.fori_loop(0, 2, step, 0)

    def own_a(u, o, half):
        s, ln = u % 2, lanes(half, H)
        return (dot(u, col_a(c, o, go, half), H, H) + p_in(s, o * 4 + go, half * H, H)
                + a2r[s, o, 1, :, ln].astype(F32) + a3r[s, o, :, ln].astype(F32))

    def s5(u):
        src = jnp.where(outer, 0, 1)

        def step(o, _):
            @pl.when(u >= 1)
            def _():
                c_t2(src, o).wait_send()

            @pl.when((u >= 1) & (o == 0))
            def _():
                pl.semaphore_wait(ct2, 1)

            @pl.when(inner)
            def _():
                c_t1(o).wait_recv()

            half = jnp.where(outer, near, far)
            t2s[o] = (own_a(u, o, half) + t1r[o].astype(F32)).astype(BF16)
            c_t2(src, o).start()
            return 0

        lax.fori_loop(0, 2, step, 0)

        @pl.when(inner & (u + 1 < n))
        def _():
            signal(ct1, zout_d)

    def rows(v):
        return pl.ds(pl.multiple_of(v * R, R), R)

    def win_a(u, o, g, half):
        return tot.at[rows(u), pl.ds(pl.multiple_of(col_a(c, o, g, half), H), H)]

    def win_b(u, q, g=0, w=WB):
        return tot.at[rows(u), pl.ds(pl.multiple_of(col_b(c, q, g), WB), w)]

    def fa_copies(u, o):
        w = win_a(u, o, go, near)
        f = fa.at[o]
        return ((f, w, fa_s.at[o, 0], g1_m.at[u], zout_d), (f, w, fa_s.at[o, 1], g1_m.at[u], zin_d),
                (f, w, fa_s.at[o, 2], g3_m.at[0, u], sn(o)), (f, w, fa_s.at[o, 3], g4_m.at[0, u], fn(o)),
                (f, w, fa_s.at[o, 4], g5_m.at[u], partner))

    def fa_done(u, o):
        for a in fa_copies(u, o):
            copy(*a).wait_send()
        pltpu.make_async_copy(fa.at[o], win_a(u, o, go, near), la_m.at[o]).wait()

    def s6(u):
        @pl.when(inner)
        def _():
            for o in range(2):
                for src in range(2):
                    c_t2(src, o).wait_recv()

            def step(o, _):
                @pl.when(u >= 1)
                def _():
                    fa_done(u, o)

                fa[o] = (own_a(u, o, near) + t2r[0, o].astype(F32) + t2r[1, o].astype(F32)).astype(BF16)
                pltpu.make_async_copy(fa.at[o], win_a(u, o, go, near), la_m.at[o]).start()
                for a in fa_copies(u, o):
                    copy(*a).start()
                return 0

            lax.fori_loop(0, 2, step, 0)

            @pl.when(u + 1 < n)
            def _():
                signal(ct2, zout_d)
                signal(ct2, zin_d)

        @pl.when(u + 2 < n)
        def _():
            for o in range(2):
                signal(ca2.at[o], fn(o))
                signal(ca3.at[o], sn(o))

    def t3(u):
        def step(d, _):
            ok = jnp.where(d == 0, up_ok, dn_ok)

            @pl.when(ok)
            def _():
                to = pick(d, up, down)

                @pl.when(u >= 1)
                def _():
                    c_b3(d, to).wait_send()
                    pl.semaphore_wait(cb3.at[d], 1)

                @pl.when(inner)
                def _():
                    c_b2(d).wait_recv()

                q = pick(d, zu, zd)
                b3s[d] = (dot(u, col_b(c, q), WA, WA) + p_in(u % 2, 8 + q) + b2r[d].astype(F32)).astype(BF16)
                c_b3(d, to).start()

            return 0

        lax.fori_loop(0, 2, step, 0)

        @pl.when(inner & (u + 1 < n))
        def _():
            signal(cb2, zout_d)
            signal(cb2, zin_d)

    def own_b(u, g):
        ln = lanes(g, WB)
        return (dot(u, col_b(c, z, g), WB, WB) + p_in(u % 2, 8 + z, g * WB, WB)
                + b3r[0, :, ln].astype(F32) + b3r[1, :, ln].astype(F32))

    def t4(u):
        @pl.when(dn_ok)
        def _():
            c_b3(0).wait_recv()

        @pl.when(up_ok)
        def _():
            c_b3(1).wait_recv()

        o = u % 2

        def step(m, _):
            @pl.when(u >= 1)
            def _():
                c_b4(o, m).wait_send()

            @pl.when((u >= 1) & (m == 0))
            def _():
                pl.semaphore_wait(cb4, 1)

            b4s[m] = own_b(u, jnp.where(m == 0, gd, gf(o))).astype(BF16)
            c_b4(o, m).start()
            return 0

        lax.fori_loop(0, 2, step, 0)

    def t5(u):
        o = u % 2

        @pl.when(u >= 1)
        def _():
            c_b5(o).wait_send()
            pl.semaphore_wait(cb5, 1)

        c_b4(o, 0).wait_recv()
        b5s[...] = (own_b(u, gs(o)) + b4r[0].astype(F32)).astype(BF16)
        c_b5(o).start()

    def fb_copies(u):
        w, o = win_b(u, z, go), u % 2
        return ((fb, w, fb_s.at[0], h1_m.at[u], sn(o)), (fb, w, fb_s.at[1], h2_m.at[0, u], fn(o)))

    def fb_local(u):
        return pltpu.make_async_copy(fb, win_b(u, z, go), lb_m)

    def t6(u):
        o = u % 2
        c_b4(o, 1).wait_recv()
        c_b5(o).wait_recv()

        @pl.when(u >= 1)
        def _():
            for a in fb_copies(u):
                copy(*a).wait_send()

        fb[...] = (own_b(u, go) + b4r[1].astype(F32) + b5r[...].astype(F32)).astype(BF16)
        fb_local(u).start()
        for a in fb_copies(u):
            copy(*a).start()

        @pl.when(u + 1 < n)
        def _():
            @pl.when(dn_ok)
            def _():
                signal(cb3.at[0], down)

            @pl.when(up_ok)
            def _():
                signal(cb3.at[1], up)

            signal(cb4, fn(1 - o))
            signal(cb5, sn(1 - o))

        @pl.when(u + 2 < n)
        def _():
            signal(cp, partner)

    def go_on(v, cond, k, src, rs, to):
        def make():
            return copy(src(v), src(v), q_s.at[k], rs(v), to)

        @pl.when(cond if cond is not True else v >= 0)
        def _():
            @pl.when(v >= 1)
            def _():
                make().wait_send()

            make().start()

    plan = []

    def op(group, cond, src, rs, to):
        plan.append((group, cond, len(plan), src, rs, to))

    def half_ops(group, cond, half, which):
        for o in range(2):
            w = functools.partial(lambda o, half, v: win_a(v, o, go, half), o, half)
            op(group, cond, w, functools.partial(lambda k, v: g3_m.at[k, v], which), sn(o))
            op(group, cond, w, functools.partial(lambda k, v: g4_m.at[k, v], which), fn(o))
            op(group, cond, w, lambda v: g5_m.at[v], partner)

    for o in range(2):
        op("q0", inner, functools.partial(lambda o, v: win_a(v, o, go, far), o), lambda v: g2_m.at[v], zout_d)
    half_ops("q0i", inner, far, 1)
    half_ops("q0o", outer, near, 0)
    half_ops("q1", outer, far, 1)
    for k, half in ((0, near), (1, far)):
        for o in range(2):
            w = functools.partial(lambda o, half, v: win_a(v, o, gs(o), half), o, half)
            op(f"q{2 + k}", True, w, functools.partial(lambda k, v: g4_m.at[2 + k, v], k), fn(o))
            op(f"q{2 + k}", True, w, lambda v: g5_m.at[v], partner)
    for o in range(2):
        for half in range(2):
            op("q4", True, functools.partial(lambda o, half, v: win_a(v, o, gf(o), half), o, half), lambda v: g5_m.at[v], partner)
            op("q5", True, functools.partial(lambda o, half, v: win_a(v, o, gd, half), o, half), lambda v: g5_m.at[v], partner)
    op("r0", True, lambda v: win_b(v, z, gs(v % 2)), lambda v: h2_m.at[1, v], None)
    block = lambda q: (lambda v: win_b(v, q, w=4 * WB))
    op("r1", up_ok, block(z), lambda v: hz_m.at[0, v], up)
    op("r1", dn_ok, block(z), lambda v: hz_m.at[1, v], down)
    op("r1", True, block(z), lambda v: h5_m.at[v], partner)
    zm2, zp2 = jnp.maximum(z - 2, 0), jnp.minimum(z + 2, 3)
    op("r2u", dn_ok & up_ok, block(zd), lambda v: hz_m.at[2, v], up)
    op("r2u", dn_ok, block(zd), lambda v: h5_m.at[v], partner)
    op("r2d", dn_ok & up_ok, block(zu), lambda v: hz_m.at[3, v], down)
    op("r2d", up_ok, block(zu), lambda v: h5_m.at[v], partner)
    op("r3u", z == 2, block(zm2), lambda v: hz_m.at[4, v], up)
    op("r3u", z >= 2, block(zm2), lambda v: h5_m.at[v], partner)
    op("r3d", z == 1, block(zp2), lambda v: hz_m.at[5, v], down)
    op("r3d", z <= 1, block(zp2), lambda v: h5_m.at[v], partner)
    op("r4", outer, block(3 - z), lambda v: h5_m.at[v], partner)

    def run(group, v):
        for g_, cond, k, src, rs, to in plan:
            if g_ == group:
                go_on(v, cond, k, src, rs, fn(v % 2) if to is None else to)

    def arrived(ref, sem):
        copy(ref, ref, q_s.at[0], sem, partner).wait_recv()

    def pair(v):
        return tot.at[rows(v), pl.ds(0, WA)]

    def q0a(v):
        arrived(pair(v), g1_m.at[v])
        run("q0", v)
        run("q0i", v)
        run("q0o", v)

    def q0b(v):
        arrived(win_b(v, 0), h1_m.at[v])
        run("r0", v)

    def q1a(v):
        @pl.when(outer)
        def _():
            arrived(pair(v), g2_m.at[v])

        run("q1", v)

    def q1b(v):
        fb_local(v).wait()
        for k in range(2):
            arrived(win_b(v, 0), h2_m.at[k, v])
        run("r1", v)

    def q2a(v):
        arrived(pair(v), g3_m.at[0, v])
        run("q2", v)

    def q3a(v):
        arrived(pair(v), g3_m.at[1, v])
        run("q3", v)

    def hop(v, up_there, down_there, k, groups):
        for there, kk, g in ((up_there, k, groups[0]), (down_there, k + 1, groups[1])):
            @pl.when(there)
            def _():
                arrived(win_b(v, 0, w=4 * WB), hz_m.at[kk, v])

            run(g, v)

    def q2b(v):
        hop(v, dn_ok, up_ok, 0, ("r2u", "r2d"))

    def q3b(v):
        hop(v, z >= 2, z <= 1, 2, ("r3u", "r3d"))

    def q4b(v):
        hop(v, z == 3, z == 0, 4, ("", "r4"))

    def q4a(v):
        for k in range(2):
            arrived(pair(v), g4_m.at[k, v])
        run("q4", v)

    def q5(v):
        for k in range(2):
            arrived(pair(v), g4_m.at[2 + k, v])
        run("q5", v)

    def all_here(v):
        arrived(tot.at[rows(v), pl.ds(0, 8 * WA)], g5_m.at[v])
        arrived(tot.at[rows(v), pl.ds(0, 16 * WB)], h5_m.at[v])

    def stage(v):
        all_here(v)
        pltpu.make_async_copy(tot.at[rows(v)], big.at[rows(v)], st_m.at[v]).start()

    @pl.when(outer)
    def _():
        t1r[...] = jnp.zeros_like(t1r)
        b1r[...] = jnp.zeros_like(b1r)
        b2r[...] = jnp.zeros_like(b2r)

    @pl.when(z == 0)
    def _():
        b3r[0] = jnp.zeros_like(b3r[0])

    @pl.when(z == 3)
    def _():
        b3r[1] = jnp.zeros_like(b3r[1])

    for kk in range(NB - 1):
        for cp_ in g_copies(kk):
            cp_.start()

    g_pieces(0, 0, NK)
    s1(0)
    cut = [NK * k // 8 for k in range(9)]

    def slot(t, _):
        def at(i, f):
            @pl.when((i >= 0) & (i < n))
            def _():
                f(i)

        def g(a, b):
            at(t + 1, lambda i: g_pieces(i, cut[a], cut[b]))

        u, v, w, e = t - 1, t - 2, t - 3, t - 4
        at(v, q0a)
        at(t - 8, q4b)
        at(u, s4)
        g(0, 1)
        at(t, t1)
        at(u, t4)
        at(t, lambda i: s2(i, 0))
        at(u, s5)
        at(v, q1b)
        at(t - 7, q4a)
        g(1, 2)
        at(u, t5)
        at(t - 7, q3a)
        at(t, lambda i: s2(i, 1))
        g(2, 3)
        at(e, q2a)
        at(e, q3b)
        g(3, 4)
        at(t, t2)
        g(4, 6)
        at(u, s6)
        at(u, t6)
        at(t, s3)
        g(6, 8)
        at(v, q1a)
        at(t - 8, q5)
        at(t, t3)
        at(v, q2b)
        at(t + 1, s1)
        at(u, q0b)
        pl.when(t == n + 1)(lambda: c_p(0).wait_send())

        pl.when((t > n) & (t <= n + S))(lambda: stage(t - n - 1))

        return 0

    lax.fori_loop(0, n + 8, slot, 0)

    last = n - 1
    for o in range(2):
        for m in range(2):
            c_a2(0, o, m).wait_send()
        c_b4(0, o).wait_send()
        c_a3(0, o).wait_send()
        c_t2(0, o).wait_send()

        @pl.when(outer)
        def _():
            c_t1(o).wait_send()

        @pl.when(inner)
        def _():
            fa_done(last, o)

        @pl.when(up_ok if o == 0 else dn_ok)
        def _():
            c_b3(o).wait_send()

    @pl.when(outer)
    def _():
        c_b1().wait_send()

    c_b2(0).wait_send()
    c_b5(0).wait_send()
    for a in fb_copies(last):
        copy(*a).wait_send()
    for g_, cond, k, src, rs, to in plan:
        def done(k=k, src=src, rs=rs):
            copy(src(last), src(last), q_s.at[k], rs(last), partner).wait_send()

        if cond is True:
            done()
        else:
            pl.when(cond)(done)

    for v in range(S, n):
        all_here(v)
    for v in range(S):
        pltpu.make_async_copy(tot.at[rows(v)], big.at[rows(v)], st_m.at[v]).wait()


N_OPS = 2 + 6 * 3 + 8 + 8 + 1 + 3 + 8 + 1


def block_sums(cfg, x, w_gate, w_up, w_down):
    n, R, D, FF, WA, H, WB, KB = (cfg[k] for k in ("n", "R", "D", "FF", "WA", "H", "WB", "KB"))
    NB = 3
    vm = lambda *s: pltpu.VMEM(s, BF16)
    dma = lambda *s: pltpu.SemaphoreType.DMA(s) if s else pltpu.SemaphoreType.DMA
    reg = lambda *s: pltpu.SemaphoreType.REGULAR(s) if s else pltpu.SemaphoreType.REGULAR
    scratch = [
        vm(3, R, FF), vm(NB, R, KB), pltpu.VMEM((R, 2 * FF), F32),
        vm(2, 2, R, WA), vm(2, 2, 2, R, WA), vm(2, R, WA), vm(2, 2, R, WA),
        vm(2, R, H), vm(2, R, H), vm(2, R, H), vm(2, 2, R, H),
        vm(R, WA), vm(R, WA), vm(R, WA), vm(2, R, WA), vm(2, R, WA), vm(2, R, WA), vm(2, R, WB), vm(2, R, WB), vm(R, WB), vm(R, WB),
        vm(2, R, H), vm(R, WB),
        dma(6), dma(NB, 3), dma(staged(cfg)), dma(), dma(2), dma(2, 2), dma(2, 2, 2), dma(2), dma(2, 2), dma(2), dma(2), dma(2), dma(2, 2),
        dma(), dma(), dma(), dma(2), dma(2), dma(2), dma(2), dma(2), dma(), dma(),
        dma(2), dma(), dma(2, 5), dma(2), dma(N_OPS), dma(n), dma(n), dma(2, n), dma(4, n), dma(n), dma(n), dma(2, n), dma(6, n), dma(n),
        reg(), reg(2), reg(2), reg(), reg(), reg(), reg(), reg(2), reg(), reg(),
    ]
    hbm = pl.BlockSpec(memory_space=pl.ANY)
    return pl.pallas_call(
        functools.partial(body, cfg),
        name="mlp_sums",
        out_shape=(jax.ShapeDtypeStruct((n * R, D), BF16), vm(FF + KB, D)),
        in_specs=[hbm] * 4,
        out_specs=(hbm, pl.BlockSpec(memory_space=pltpu.VMEM)),
        scratch_shapes=scratch,
        compiler_params=pltpu.CompilerParams(has_side_effects=True, vmem_limit_bytes=18_000_000),
    )(x, w_gate, w_up, w_down)


def place(cfg, total, big):
    n, R, D = (cfg[k] for k in ("n", "R", "D"))
    S = staged(cfg)
    K = 4

    def kernel(t_ref, big_ref, o_ref, buf, in_m, out_m, st_m):
        def whole(v):
            rows = pl.ds(v * R, R)
            return pltpu.make_async_copy(big_ref.at[rows], o_ref.at[rows], st_m.at[v])

        def piece(i):
            return pl.ds(S * R + i * (R // K), R // K)

        last = (n - S) * K
        ins = [pltpu.make_async_copy(t_ref.at[piece(i)], buf.at[i], in_m.at[i]) for i in range(last)]
        outs = [pltpu.make_async_copy(buf.at[i], o_ref.at[piece(i)], out_m.at[i]) for i in range(last)]
        for cp in ins:
            cp.start()
        for v in range(S):
            whole(v).start()
        for there, back in zip(ins, outs):
            there.wait()
            back.start()
        for cp in outs:
            cp.wait()
        for v in range(S):
            whole(v).wait()

    hbm, dma = pl.BlockSpec(memory_space=pl.ANY), pltpu.SemaphoreType.DMA
    parts = (n - S) * K
    return pl.pallas_call(
        kernel,
        name="place",
        out_shape=jax.ShapeDtypeStruct((n * R, D), BF16),
        in_specs=[hbm, pl.BlockSpec(memory_space=pltpu.VMEM)],
        out_specs=hbm,
        scratch_shapes=[pltpu.VMEM((parts, R // K, D), BF16), dma((parts,)), dma((parts,)), dma((S,))],
        compiler_params=pltpu.CompilerParams(vmem_limit_bytes=14_000_000),
    )(total, pltpu.with_memory_space_constraint(big, pltpu.VMEM))


def build(mesh, chunk, pieces):
    def step(x, w_gate, w_up, w_down):
        cfg = dims(x.shape[0], x.shape[1], w_gate.shape[1], chunk, pieces)
        return place(cfg, *block_sums(cfg, x, w_gate, w_up, w_down))

    return jax.shard_map(
        step,
        mesh=mesh,
        in_specs=(P("dp", None), P(None, "tp"), P(None, "tp"), P("tp", None)),
        out_specs=P("dp", None),
        check_vma=False,
    )


def solution(mesh):
    return build(mesh, 256, 12)
```

```python
import functools
import math

import jax
import jax.numpy as jnp
from jax import lax
from jax.experimental import pallas as pl
from jax.experimental.pallas import tpu as pltpu
from jax.sharding import PartitionSpec as P

F32 = jnp.float32
BF16 = jnp.bfloat16
MESH = pl.DeviceIdType.MESH


def dims(rows, d, ff, chunk, pieces):
    wa = d // 24
    return dict(n=rows // chunk, R=chunk, D=d, FF=ff, WA=wa, H=wa // 2, WB=wa // 4, NK=pieces, KB=d // pieces)


def staged(cfg):
    return min((cfg["FF"] + cfg["KB"]) // cfg["R"], cfg["n"] - 1)


def body(cfg, x_ref, wg_ref, wu_ref, wdh_ref, tot, big, h, xb, acc, a2s, a2r, a3s, a3r, t1s, t1r, t2s, t2r,
         b1s, b1r, b2s, b2r, b3s, b3r, b4s, b4r, b5s, b5r, fa, fb,
         wd_m, g_m, st_m, p_s, p_m, a2_s, a2_m, a3_s, a3_m, t1_s, t1_m, t2_s, t2_m, b1_s, b1_m, b2_s, b2_m, b3_s, b3_m, b4_s, b4_m, b5_s, b5_m,
         la_m, lb_m, fa_s, fb_s, q_s, g1_m, g2_m, g3_m, g4_m, g5_m, h1_m, h2_m, hz_m, h5_m,
         cp, ca2, ca3, ct1, ct2, cb1, cb2, cb3, cb4, cb5):
    n, R, D, FF, WA, H, WB, NK, KB = (cfg[k] for k in ("n", "R", "D", "FF", "WA", "H", "WB", "NK", "KB"))
    NB = xb.shape[0]
    S = staged(cfg)
    me = lax.axis_index("tp")
    dp = lax.axis_index("dp")
    x, y, z, c = me // 16, (me // 8) % 2, (me // 2) % 4, me % 2

    def dev(x, y, z, c):
        return (dp, ((x * 2 + y) * 4 + z) * 2 + c)

    outer = (z == 0) | (z == 3)
    inner = jnp.logical_not(outer)
    up_ok, dn_ok = z < 3, z > 0
    zu, zd = jnp.minimum(z + 1, 3), jnp.maximum(z - 1, 0)
    zin = jnp.where(outer, jnp.where(z == 0, 1, 2), 3 - z)
    zout = jnp.where(z < 2, 0, 3)
    near = jnp.where(z < 2, 0, 1)
    far = 1 - near
    partner = dev(x, y, z, 1 - c)
    xn, yn = dev(1 - x, y, z, c), dev(x, 1 - y, z, c)
    up, down, zin_d, zout_d = dev(x, y, zu, c), dev(x, y, zd, c), dev(x, y, zin, c), dev(x, y, zout, c)
    go, gx, gy, gd = x * 2 + y, (1 - x) * 2 + y, x * 2 + 1 - y, (1 - x) * 2 + 1 - y

    def pick(order, a, b):
        first = order == 0
        return jax.tree.map(lambda p, q: jnp.where(first, p, q), a, b)

    def fn(order):
        return pick(order, xn, yn)

    def sn(order):
        return pick(order, yn, xn)

    def gf(order):
        return pick(order, gx, gy)

    def gs(order):
        return pick(order, gy, gx)

    def copy(src, dst, ss, rs, to):
        return pltpu.make_async_remote_copy(src, dst, ss, rs, device_id=to, device_id_type=MESH)

    def signal(sem, to):
        pl.semaphore_signal(sem, inc=1, device_id=to, device_id_type=MESH)

    def col_a(core, order, g, half=0):
        return core * (8 * WA) + order * (4 * WA) + g * WA + half * H

    def col_b(core, q, g=0):
        return 16 * WA + core * (16 * WB) + q * (4 * WB) + g * WB

    def lanes(i, w):
        return pl.ds(pl.multiple_of(i * w, w), w)

    def dot(i, col, w, unit):
        return jnp.dot(h[i % 3], big[pl.ds(0, FF), pl.ds(pl.multiple_of(col, unit), w)], preferred_element_type=F32)

    def weights(b, off, w):
        return pl.ds(FF, KB), pl.ds(pl.multiple_of(b * 2 * FF + off, FF), w)

    def tile(k, off=0, w=WA):
        across, first = (D - NB * 2 * FF) // WA, NB * 2 * FF
        row, col = FF + k // across * R, first + k % across * WA + off
        return (pl.ds(pl.multiple_of(row, math.gcd(FF, R)), R), pl.ds(pl.multiple_of(col, math.gcd(first, WB)), w))

    def p_in(s, j, off=0, w=WA):
        return big[tile(s * 12 + j, off, w)].astype(F32)

    def p_tile(k):
        return big.at[tile(k)]

    def c_p(s):
        every = big.at[pl.ds(0, R), pl.ds(0, 12 * WA)]
        return copy(every, every, p_s, p_m.at[s], partner)

    def c_a2(s, o, m):
        return copy(a2s.at[o, m], a2r.at[s, o, m], a2_s.at[o, m], a2_m.at[s, o, m], fn(o))

    def c_a3(s, o):
        return copy(a3s.at[o], a3r.at[s, o], a3_s.at[o], a3_m.at[s, o], sn(o))

    def c_t1(o):
        return copy(t1s.at[o], t1r.at[o], t1_s.at[o], t1_m.at[o], zin_d)

    def c_t2(src, o):
        return copy(t2s.at[o], t2r.at[src, o], t2_s.at[o], t2_m.at[src, o], zin_d)

    def c_b1():
        return copy(b1s, b1r, b1_s, b1_m, zin_d)

    def c_b2(d):
        return copy(b2s, b2r.at[d], b2_s, b2_m.at[d], zin_d)

    def c_b3(d, to=up):
        return copy(b3s.at[d], b3r.at[d], b3_s.at[d], b3_m.at[d], to)

    def c_b4(o, m):
        return copy(b4s.at[m], b4r.at[m], b4_s.at[m], b4_m.at[m], fn(o))

    def c_b5(o):
        return copy(b5s, b5r, b5_s, b5_m, sn(o))

    def g_copies(kk):
        i, k, b = kk // NK, kk % NK, kk % NB
        rows, ks = pl.ds(pl.multiple_of(i * R, R), R), pl.ds(pl.multiple_of(k * KB, KB), KB)
        return (pltpu.make_async_copy(x_ref.at[rows, ks], xb.at[b], g_m.at[b, 0]),
                pltpu.make_async_copy(wg_ref.at[ks], big.at[weights(b, 0, FF)], g_m.at[b, 1]),
                pltpu.make_async_copy(wu_ref.at[ks], big.at[weights(b, FF, FF)], g_m.at[b, 2]))

    def wd_copy(k):
        core, m = jnp.where(k < 3, 1 - c, c), k % 3
        off = jnp.where(m < 2, col_a(core, m, 0), col_b(core, 0))
        cols = pl.ds(pl.multiple_of(off, 4 * WA), 4 * WA)
        return pltpu.make_async_copy(wdh_ref.at[:, cols], big.at[pl.ds(0, FF), cols], wd_m.at[k])

    def g_pieces(i, k0, k1):
        def step(k, _):
            kk = i * NK + k
            b = kk % NB
            for cp_ in g_copies(kk):
                cp_.wait()

            @pl.when(kk == NK - 1)
            def _():
                for p in range(6):
                    wd_copy(p).start()

            @pl.when((kk + NB - 1 < n * NK))
            def _():
                for cp_ in g_copies(kk + NB - 1):
                    cp_.start()

            @pl.when(k == 0)
            def _():
                acc[...] = jnp.zeros_like(acc)

            acc[...] += jnp.dot(xb[b], big[weights(b, 0, 2 * FF)], preferred_element_type=F32)
            return 0

        lax.fori_loop(k0, k1, step, 0)
        if k1 == NK:
            h[i % 3] = (jax.nn.silu(acc[:, :FF]) * acc[:, FF:]).astype(BF16)

    def s1(t):
        @pl.when(t >= 1)
        def _():
            c_p(0).wait_send()

        @pl.when(t >= 2)
        def _():
            pl.semaphore_wait(cp, 1)

        def step(j, _):
            @pl.when((t == 0) & (j % 2 == 0))
            def _():
                wd_copy(j // 2).wait()

            v = dot(t, jnp.where(j < 4, col_a(1 - c, 0, 2 * j), col_b(1 - c, 2 * j - 8)), 2 * WA, WA).astype(BF16)
            for k in range(2):
                m = j * 2 + k
                p_tile(24 + m)[...] = v[:, k * WA:(k + 1) * WA]
                copy(p_tile(24 + m), p_tile(t % 2 * 12 + m), p_s, p_m.at[t % 2], partner).start()
            return 0

        lax.fori_loop(0, 6, step, 0)

    def s2(t, m):
        def step(o, _):
            @pl.when(t >= 1)
            def _():
                c_a2(0, o, m).wait_send()

            if m == 0:
                @pl.when(t >= 2)
                def _():
                    pl.semaphore_wait(ca2.at[o], 1)

            g = gf(o) if m else gd
            v = dot(t, col_a(c, o, g), WA, WA) + p_in(t % 2, o * 4 + g)
            a2s[o, m] = v.astype(BF16)
            c_a2(t % 2, o, m).start()
            return 0

        lax.fori_loop(0, 2, step, 0)

    def s3(t):
        def step(o, _):
            @pl.when(t >= 1)
            def _():
                c_a3(0, o).wait_send()

            @pl.when(t >= 2)
            def _():
                pl.semaphore_wait(ca3.at[o], 1)

            c_a2(t % 2, o, 0).wait_recv()
            g = gs(o)
            v = dot(t, col_a(c, o, g), WA, WA) + p_in(t % 2, o * 4 + g) + a2r[t % 2, o, 0].astype(F32)
            a3s[o] = v.astype(BF16)
            c_a3(t % 2, o).start()
            return 0

        lax.fori_loop(0, 2, step, 0)

    def t1(t):
        @pl.when(t == 0)
        def _():
            for p in range(3, 6):
                wd_copy(p).wait()

        c_p(t % 2).wait_recv()

        @pl.when(outer)
        def _():
            @pl.when(t >= 1)
            def _():
                c_b1().wait_send()
                pl.semaphore_wait(cb1, 1)

            q = 3 - z
            b1s[...] = (dot(t, col_b(c, q), WA, WA) + p_in(t % 2, 8 + q)).astype(BF16)
            c_b1().start()

    def t2(t):
        @pl.when(t >= 1)
        def _():
            c_b2(0).wait_send()
            pl.semaphore_wait(cb2, 1)

        @pl.when(inner)
        def _():
            c_b1().wait_recv()

        q = (z + 2) % 4
        b2s[...] = (dot(t, col_b(c, q), WA, WA) + p_in(t % 2, 8 + q) + b1r[...].astype(F32)).astype(BF16)
        d = jnp.where(z < 2, 0, 1)
        c_b2(d).start()

        @pl.when(inner & (t + 1 < n))
        def _():
            signal(cb1, zout_d)

    def s4(u):
        for o in range(2):
            c_a3(u % 2, o).wait_recv()
            c_a2(u % 2, o, 1).wait_recv()

        @pl.when(outer)
        def _():
            def step(o, _):
                @pl.when(u >= 1)
                def _():
                    c_t1(o).wait_send()

                @pl.when((u >= 1) & (o == 0))
                def _():
                    pl.semaphore_wait(ct1, 1)

                t1s[o] = own_a(u, o, far).astype(BF16)
                c_t1(o).start()
                return 0

            lax.fori_loop(0, 2, step, 0)

    def own_a(u, o, half):
        s, ln = u % 2, lanes(half, H)
        return (dot(u, col_a(c, o, go, half), H, H) + p_in(s, o * 4 + go, half * H, H)
                + a2r[s, o, 1, :, ln].astype(F32) + a3r[s, o, :, ln].astype(F32))

    def s5(u):
        src = jnp.where(outer, 0, 1)

        def step(o, _):
            @pl.when(u >= 1)
            def _():
                c_t2(src, o).wait_send()

            @pl.when((u >= 1) & (o == 0))
            def _():
                pl.semaphore_wait(ct2, 1)

            @pl.when(inner)
            def _():
                c_t1(o).wait_recv()

            half = jnp.where(outer, near, far)
            t2s[o] = (own_a(u, o, half) + t1r[o].astype(F32)).astype(BF16)
            c_t2(src, o).start()
            return 0

        lax.fori_loop(0, 2, step, 0)

        @pl.when(inner & (u + 1 < n))
        def _():
            signal(ct1, zout_d)

    def rows(v):
        return pl.ds(pl.multiple_of(v * R, R), R)

    def win_a(u, o, g, half):
        return tot.at[rows(u), pl.ds(pl.multiple_of(col_a(c, o, g, half), H), H)]

    def win_b(u, q, g=0, w=WB):
        return tot.at[rows(u), pl.ds(pl.multiple_of(col_b(c, q, g), WB), w)]

    def fa_copies(u, o):
        w = win_a(u, o, go, near)
        f = fa.at[o]
        return ((f, w, fa_s.at[o, 0], g1_m.at[u], zout_d), (f, w, fa_s.at[o, 1], g1_m.at[u], zin_d),
                (f, w, fa_s.at[o, 2], g3_m.at[0, u], sn(o)), (f, w, fa_s.at[o, 3], g4_m.at[0, u], fn(o)),
                (f, w, fa_s.at[o, 4], g5_m.at[u], partner))

    def fa_done(u, o):
        for a in fa_copies(u, o):
            copy(*a).wait_send()
        pltpu.make_async_copy(fa.at[o], win_a(u, o, go, near), la_m.at[o]).wait()

    def s6(u):
        @pl.when(inner)
        def _():
            for o in range(2):
                for src in range(2):
                    c_t2(src, o).wait_recv()

            def step(o, _):
                @pl.when(u >= 1)
                def _():
                    fa_done(u, o)

                fa[o] = (own_a(u, o, near) + t2r[0, o].astype(F32) + t2r[1, o].astype(F32)).astype(BF16)
                pltpu.make_async_copy(fa.at[o], win_a(u, o, go, near), la_m.at[o]).start()
                for a in fa_copies(u, o):
                    copy(*a).start()
                return 0

            lax.fori_loop(0, 2, step, 0)

            @pl.when(u + 1 < n)
            def _():
                signal(ct2, zout_d)
                signal(ct2, zin_d)

        @pl.when(u + 2 < n)
        def _():
            for o in range(2):
                signal(ca2.at[o], fn(o))
                signal(ca3.at[o], sn(o))

    def t3(u):
        def step(d, _):
            ok = jnp.where(d == 0, up_ok, dn_ok)

            @pl.when(ok)
            def _():
                to = pick(d, up, down)

                @pl.when(u >= 1)
                def _():
                    c_b3(d, to).wait_send()
                    pl.semaphore_wait(cb3.at[d], 1)

                @pl.when(inner)
                def _():
                    c_b2(d).wait_recv()

                q = pick(d, zu, zd)
                b3s[d] = (dot(u, col_b(c, q), WA, WA) + p_in(u % 2, 8 + q) + b2r[d].astype(F32)).astype(BF16)
                c_b3(d, to).start()

            return 0

        lax.fori_loop(0, 2, step, 0)

        @pl.when(inner & (u + 1 < n))
        def _():
            signal(cb2, zout_d)
            signal(cb2, zin_d)

    def own_b(u, g):
        ln = lanes(g, WB)
        return (dot(u, col_b(c, z, g), WB, WB) + p_in(u % 2, 8 + z, g * WB, WB)
                + b3r[0, :, ln].astype(F32) + b3r[1, :, ln].astype(F32))

    def t4(u):
        @pl.when(dn_ok)
        def _():
            c_b3(0).wait_recv()

        @pl.when(up_ok)
        def _():
            c_b3(1).wait_recv()

        o = u % 2

        def step(m, _):
            @pl.when(u >= 1)
            def _():
                c_b4(o, m).wait_send()

            @pl.when((u >= 1) & (m == 0))
            def _():
                pl.semaphore_wait(cb4, 1)

            b4s[m] = own_b(u, jnp.where(m == 0, gd, gf(o))).astype(BF16)
            c_b4(o, m).start()
            return 0

        lax.fori_loop(0, 2, step, 0)

    def t5(u):
        o = u % 2

        @pl.when(u >= 1)
        def _():
            c_b5(o).wait_send()
            pl.semaphore_wait(cb5, 1)

        c_b4(o, 0).wait_recv()
        b5s[...] = (own_b(u, gs(o)) + b4r[0].astype(F32)).astype(BF16)
        c_b5(o).start()

    def fb_copies(u):
        w, o = win_b(u, z, go), u % 2
        return ((fb, w, fb_s.at[0], h1_m.at[u], sn(o)), (fb, w, fb_s.at[1], h2_m.at[0, u], fn(o)))

    def fb_local(u):
        return pltpu.make_async_copy(fb, win_b(u, z, go), lb_m)

    def t6(u):
        o = u % 2
        c_b4(o, 1).wait_recv()
        c_b5(o).wait_recv()

        @pl.when(u >= 1)
        def _():
            for a in fb_copies(u):
                copy(*a).wait_send()

        fb[...] = (own_b(u, go) + b4r[1].astype(F32) + b5r[...].astype(F32)).astype(BF16)
        fb_local(u).start()
        for a in fb_copies(u):
            copy(*a).start()

        @pl.when(u + 1 < n)
        def _():
            @pl.when(dn_ok)
            def _():
                signal(cb3.at[0], down)

            @pl.when(up_ok)
            def _():
                signal(cb3.at[1], up)

            signal(cb4, fn(1 - o))
            signal(cb5, sn(1 - o))

        @pl.when(u + 2 < n)
        def _():
            signal(cp, partner)

    def go_on(v, cond, k, src, rs, to):
        def make():
            return copy(src(v), src(v), q_s.at[k], rs(v), to)

        @pl.when(cond if cond is not True else v >= 0)
        def _():
            @pl.when(v >= 1)
            def _():
                make().wait_send()

            make().start()

    plan = []

    def op(group, cond, src, rs, to):
        plan.append((group, cond, len(plan), src, rs, to))

    def half_ops(group, cond, half, which):
        for o in range(2):
            w = functools.partial(lambda o, half, v: win_a(v, o, go, half), o, half)
            op(group, cond, w, functools.partial(lambda k, v: g3_m.at[k, v], which), sn(o))
            op(group, cond, w, functools.partial(lambda k, v: g4_m.at[k, v], which), fn(o))
            op(group, cond, w, lambda v: g5_m.at[v], partner)

    for o in range(2):
        op("q0", inner, functools.partial(lambda o, v: win_a(v, o, go, far), o), lambda v: g2_m.at[v], zout_d)
    half_ops("q0i", inner, far, 1)
    half_ops("q0o", outer, near, 0)
    half_ops("q1", outer, far, 1)
    for k, half in ((0, near), (1, far)):
        for o in range(2):
            w = functools.partial(lambda o, half, v: win_a(v, o, gs(o), half), o, half)
            op(f"q{2 + k}", True, w, functools.partial(lambda k, v: g4_m.at[2 + k, v], k), fn(o))
            op(f"q{2 + k}", True, w, lambda v: g5_m.at[v], partner)
    for o in range(2):
        for half in range(2):
            op("q4", True, functools.partial(lambda o, half, v: win_a(v, o, gf(o), half), o, half), lambda v: g5_m.at[v], partner)
            op("q5", True, functools.partial(lambda o, half, v: win_a(v, o, gd, half), o, half), lambda v: g5_m.at[v], partner)
    op("r0", True, lambda v: win_b(v, z, gs(v % 2)), lambda v: h2_m.at[1, v], None)
    block = lambda q: (lambda v: win_b(v, q, w=4 * WB))
    op("r1", up_ok, block(z), lambda v: hz_m.at[0, v], up)
    op("r1", dn_ok, block(z), lambda v: hz_m.at[1, v], down)
    op("r1", True, block(z), lambda v: h5_m.at[v], partner)
    zm2, zp2 = jnp.maximum(z - 2, 0), jnp.minimum(z + 2, 3)
    op("r2u", dn_ok & up_ok, block(zd), lambda v: hz_m.at[2, v], up)
    op("r2u", dn_ok, block(zd), lambda v: h5_m.at[v], partner)
    op("r2d", dn_ok & up_ok, block(zu), lambda v: hz_m.at[3, v], down)
    op("r2d", up_ok, block(zu), lambda v: h5_m.at[v], partner)
    op("r3u", z == 2, block(zm2), lambda v: hz_m.at[4, v], up)
    op("r3u", z >= 2, block(zm2), lambda v: h5_m.at[v], partner)
    op("r3d", z == 1, block(zp2), lambda v: hz_m.at[5, v], down)
    op("r3d", z <= 1, block(zp2), lambda v: h5_m.at[v], partner)
    op("r4", outer, block(3 - z), lambda v: h5_m.at[v], partner)

    def run(group, v):
        for g_, cond, k, src, rs, to in plan:
            if g_ == group:
                go_on(v, cond, k, src, rs, fn(v % 2) if to is None else to)

    def arrived(ref, sem):
        copy(ref, ref, q_s.at[0], sem, partner).wait_recv()

    def pair(v):
        return tot.at[rows(v), pl.ds(0, WA)]

    def q0a(v):
        arrived(pair(v), g1_m.at[v])
        run("q0", v)
        run("q0i", v)
        run("q0o", v)

    def q0b(v):
        arrived(win_b(v, 0), h1_m.at[v])
        run("r0", v)

    def q1a(v):
        @pl.when(outer)
        def _():
            arrived(pair(v), g2_m.at[v])

        run("q1", v)

    def q1b(v):
        fb_local(v).wait()
        for k in range(2):
            arrived(win_b(v, 0), h2_m.at[k, v])
        run("r1", v)

    def q2a(v):
        arrived(pair(v), g3_m.at[0, v])
        run("q2", v)

    def q3a(v):
        arrived(pair(v), g3_m.at[1, v])
        run("q3", v)

    def hop(v, up_there, down_there, k, groups):
        for there, kk, g in ((up_there, k, groups[0]), (down_there, k + 1, groups[1])):
            @pl.when(there)
            def _():
                arrived(win_b(v, 0, w=4 * WB), hz_m.at[kk, v])

            run(g, v)

    def q2b(v):
        hop(v, dn_ok, up_ok, 0, ("r2u", "r2d"))

    def q3b(v):
        hop(v, z >= 2, z <= 1, 2, ("r3u", "r3d"))

    def q4b(v):
        hop(v, z == 3, z == 0, 4, ("", "r4"))

    def q4a(v):
        for k in range(2):
            arrived(pair(v), g4_m.at[k, v])
        run("q4", v)

    def q5(v):
        for k in range(2):
            arrived(pair(v), g4_m.at[2 + k, v])
        run("q5", v)

    def all_here(v):
        arrived(tot.at[rows(v), pl.ds(0, 8 * WA)], g5_m.at[v])
        arrived(tot.at[rows(v), pl.ds(0, 16 * WB)], h5_m.at[v])

    def stage(v):
        all_here(v)
        pltpu.make_async_copy(tot.at[rows(v)], big.at[rows(v)], st_m.at[v]).start()

    @pl.when(outer)
    def _():
        t1r[...] = jnp.zeros_like(t1r)
        b1r[...] = jnp.zeros_like(b1r)
        b2r[...] = jnp.zeros_like(b2r)

    @pl.when(z == 0)
    def _():
        b3r[0] = jnp.zeros_like(b3r[0])

    @pl.when(z == 3)
    def _():
        b3r[1] = jnp.zeros_like(b3r[1])

    for kk in range(NB - 1):
        for cp_ in g_copies(kk):
            cp_.start()

    g_pieces(0, 0, NK)
    s1(0)
    cut = [NK * k // 8 for k in range(9)]

    def slot(t, _):
        def at(i, f):
            @pl.when((i >= 0) & (i < n))
            def _():
                f(i)

        def g(a, b):
            at(t + 1, lambda i: g_pieces(i, cut[a], cut[b]))

        u, v, w, e = t - 1, t - 2, t - 3, t - 4
        at(v, q0a)
        at(t - 8, q4b)
        at(u, s4)
        g(0, 1)
        at(t, t1)
        at(u, t4)
        at(t, lambda i: s2(i, 0))
        at(u, s5)
        at(v, q1b)
        at(t - 7, q4a)
        g(1, 2)
        at(u, t5)
        at(t - 7, q3a)
        at(t, lambda i: s2(i, 1))
        g(2, 3)
        at(e, q2a)
        at(e, q3b)
        g(3, 4)
        at(t, t2)
        g(4, 6)
        at(u, s6)
        at(u, t6)
        at(t, s3)
        g(6, 8)
        at(v, q1a)
        at(t - 8, q5)
        at(t, t3)
        at(v, q2b)
        at(t + 1, s1)
        at(u, q0b)
        pl.when(t == n + 1)(lambda: c_p(0).wait_send())

        pl.when((t > n) & (t <= n + S))(lambda: stage(t - n - 1))

        return 0

    lax.fori_loop(0, n + 8, slot, 0)

    last = n - 1
    for o in range(2):
        for m in range(2):
            c_a2(0, o, m).wait_send()
        c_b4(0, o).wait_send()
        c_a3(0, o).wait_send()
        c_t2(0, o).wait_send()

        @pl.when(outer)
        def _():
            c_t1(o).wait_send()

        @pl.when(inner)
        def _():
            fa_done(last, o)

        @pl.when(up_ok if o == 0 else dn_ok)
        def _():
            c_b3(o).wait_send()

    @pl.when(outer)
    def _():
        c_b1().wait_send()

    c_b2(0).wait_send()
    c_b5(0).wait_send()
    for a in fb_copies(last):
        copy(*a).wait_send()
    for g_, cond, k, src, rs, to in plan:
        def done(k=k, src=src, rs=rs):
            copy(src(last), src(last), q_s.at[k], rs(last), partner).wait_send()

        if cond is True:
            done()
        else:
            pl.when(cond)(done)

    for v in range(S, n):
        all_here(v)
    for v in range(S):
        pltpu.make_async_copy(tot.at[rows(v)], big.at[rows(v)], st_m.at[v]).wait()


N_OPS = 2 + 6 * 3 + 8 + 8 + 1 + 3 + 8 + 1


def block_sums(cfg, x, w_gate, w_up, w_down):
    n, R, D, FF, WA, H, WB, KB = (cfg[k] for k in ("n", "R", "D", "FF", "WA", "H", "WB", "KB"))
    NB = 3
    vm = lambda *s: pltpu.VMEM(s, BF16)
    dma = lambda *s: pltpu.SemaphoreType.DMA(s) if s else pltpu.SemaphoreType.DMA
    reg = lambda *s: pltpu.SemaphoreType.REGULAR(s) if s else pltpu.SemaphoreType.REGULAR
    scratch = [
        vm(3, R, FF), vm(NB, R, KB), pltpu.VMEM((R, 2 * FF), F32),
        vm(2, 2, R, WA), vm(2, 2, 2, R, WA), vm(2, R, WA), vm(2, 2, R, WA),
        vm(2, R, H), vm(2, R, H), vm(2, R, H), vm(2, 2, R, H),
        vm(R, WA), vm(R, WA), vm(R, WA), vm(2, R, WA), vm(2, R, WA), vm(2, R, WA), vm(2, R, WB), vm(2, R, WB), vm(R, WB), vm(R, WB),
        vm(2, R, H), vm(R, WB),
        dma(6), dma(NB, 3), dma(staged(cfg)), dma(), dma(2), dma(2, 2), dma(2, 2, 2), dma(2), dma(2, 2), dma(2), dma(2), dma(2), dma(2, 2),
        dma(), dma(), dma(), dma(2), dma(2), dma(2), dma(2), dma(2), dma(), dma(),
        dma(2), dma(), dma(2, 5), dma(2), dma(N_OPS), dma(n), dma(n), dma(2, n), dma(4, n), dma(n), dma(n), dma(2, n), dma(6, n), dma(n),
        reg(), reg(2), reg(2), reg(), reg(), reg(), reg(), reg(2), reg(), reg(),
    ]
    hbm = pl.BlockSpec(memory_space=pl.ANY)
    return pl.pallas_call(
        functools.partial(body, cfg),
        name="mlp_sums",
        out_shape=(jax.ShapeDtypeStruct((n * R, D), BF16), vm(FF + KB, D)),
        in_specs=[hbm] * 4,
        out_specs=(hbm, pl.BlockSpec(memory_space=pltpu.VMEM)),
        scratch_shapes=scratch,
        compiler_params=pltpu.CompilerParams(has_side_effects=True, vmem_limit_bytes=18_000_000),
    )(x, w_gate, w_up, w_down)


def place(cfg, total, big):
    n, R, D = (cfg[k] for k in ("n", "R", "D"))
    S = staged(cfg)
    K = 4

    def kernel(t_ref, big_ref, o_ref, buf, in_m, out_m, st_m):
        def whole(v):
            rows = pl.ds(v * R, R)
            return pltpu.make_async_copy(big_ref.at[rows], o_ref.at[rows], st_m.at[v])

        def piece(i):
            return pl.ds(S * R + i * (R // K), R // K)

        last = (n - S) * K
        ins = [pltpu.make_async_copy(t_ref.at[piece(i)], buf.at[i], in_m.at[i]) for i in range(last)]
        outs = [pltpu.make_async_copy(buf.at[i], o_ref.at[piece(i)], out_m.at[i]) for i in range(last)]
        for cp in ins:
            cp.start()
        for v in range(S):
            whole(v).start()
        for there, back in zip(ins, outs):
            there.wait()
            back.start()
        for cp in outs:
            cp.wait()
        for v in range(S):
            whole(v).wait()

    hbm, dma = pl.BlockSpec(memory_space=pl.ANY), pltpu.SemaphoreType.DMA
    parts = (n - S) * K
    return pl.pallas_call(
        kernel,
        name="place",
        out_shape=jax.ShapeDtypeStruct((n * R, D), BF16),
        in_specs=[hbm, pl.BlockSpec(memory_space=pltpu.VMEM)],
        out_specs=hbm,
        scratch_shapes=[pltpu.VMEM((parts, R // K, D), BF16), dma((parts,)), dma((parts,)), dma((S,))],
        compiler_params=pltpu.CompilerParams(vmem_limit_bytes=14_000_000),
    )(total, pltpu.with_memory_space_constraint(big, pltpu.VMEM))


def build(mesh, chunk, pieces):
    def step(x, w_gate, w_up, w_down):
        cfg = dims(x.shape[0], x.shape[1], w_gate.shape[1], chunk, pieces)
        return place(cfg, *block_sums(cfg, x, w_gate, w_up, w_down))

    return jax.shard_map(
        step,
        mesh=mesh,
        in_specs=(P("dp", None), P(None, "tp"), P(None, "tp"), P("tp", None)),
        out_specs=P("dp", None),
        check_vma=False,
    )


def solution(mesh):
    return build(mesh, 256, 12)
```

```python
import functools
import math

import jax
import jax.numpy as jnp
from jax import lax
from jax.experimental import pallas as pl
from jax.experimental.pallas import tpu as pltpu
from jax.sharding import PartitionSpec as P

F32 = jnp.float32
BF16 = jnp.bfloat16
MESH = pl.DeviceIdType.MESH


def dims(rows, d, ff, chunk, pieces):
    wa = d // 24
    return dict(n=rows // chunk, R=chunk, D=d, FF=ff, WA=wa, H=wa // 2, WB=wa // 4, NK=pieces, KB=d // pieces)


def staged(cfg):
    return min((cfg["FF"] + cfg["KB"]) // cfg["R"], cfg["n"] - 1)


def body(cfg, x_ref, wg_ref, wu_ref, wdh_ref, tot, big, h, xb, acc, a2s, a2r, a3s, a3r, t1s, t1r, t2s, t2r,
         b1s, b1r, b2s, b2r, b3s, b3r, b4s, b4r, b5s, b5r, fa, fb,
         wd_m, g_m, st_m, p_s, p_m, a2_s, a2_m, a3_s, a3_m, t1_s, t1_m, t2_s, t2_m, b1_s, b1_m, b2_s, b2_m, b3_s, b3_m, b4_s, b4_m, b5_s, b5_m,
         la_m, lb_m, fa_s, fb_s, q_s, g1_m, g2_m, g3_m, g4_m, g5_m, h1_m, h2_m, hz_m, h5_m,
         cp, ca2, ca3, ct1, ct2, cb1, cb2, cb3, cb4, cb5):
    n, R, D, FF, WA, H, WB, NK, KB = (cfg[k] for k in ("n", "R", "D", "FF", "WA", "H", "WB", "NK", "KB"))
    NB = xb.shape[0]
    S = staged(cfg)
    me = lax.axis_index("tp")
    dp = lax.axis_index("dp")
    x, y, z, c = me // 16, (me // 8) % 2, (me // 2) % 4, me % 2

    def dev(x, y, z, c):
        return (dp, ((x * 2 + y) * 4 + z) * 2 + c)

    outer = (z == 0) | (z == 3)
    inner = jnp.logical_not(outer)
    up_ok, dn_ok = z < 3, z > 0
    zu, zd = jnp.minimum(z + 1, 3), jnp.maximum(z - 1, 0)
    zin = jnp.where(outer, jnp.where(z == 0, 1, 2), 3 - z)
    zout = jnp.where(z < 2, 0, 3)
    near = jnp.where(z < 2, 0, 1)
    far = 1 - near
    partner = dev(x, y, z, 1 - c)
    xn, yn = dev(1 - x, y, z, c), dev(x, 1 - y, z, c)
    up, down, zin_d, zout_d = dev(x, y, zu, c), dev(x, y, zd, c), dev(x, y, zin, c), dev(x, y, zout, c)
    go, gx, gy, gd = x * 2 + y, (1 - x) * 2 + y, x * 2 + 1 - y, (1 - x) * 2 + 1 - y

    def pick(order, a, b):
        first = order == 0
        return jax.tree.map(lambda p, q: jnp.where(first, p, q), a, b)

    def fn(order):
        return pick(order, xn, yn)

    def sn(order):
        return pick(order, yn, xn)

    def gf(order):
        return pick(order, gx, gy)

    def gs(order):
        return pick(order, gy, gx)

    def copy(src, dst, ss, rs, to):
        return pltpu.make_async_remote_copy(src, dst, ss, rs, device_id=to, device_id_type=MESH)

    def signal(sem, to):
        pl.semaphore_signal(sem, inc=1, device_id=to, device_id_type=MESH)

    def col_a(core, order, g, half=0):
        return core * (8 * WA) + order * (4 * WA) + g * WA + half * H

    def col_b(core, q, g=0):
        return 16 * WA + core * (16 * WB) + q * (4 * WB) + g * WB

    def lanes(i, w):
        return pl.ds(pl.multiple_of(i * w, w), w)

    def dot(i, col, w, unit):
        return jnp.dot(h[i % 3], big[pl.ds(0, FF), pl.ds(pl.multiple_of(col, unit), w)], preferred_element_type=F32)

    def weights(b, off, w):
        return pl.ds(FF, KB), pl.ds(pl.multiple_of(b * 2 * FF + off, FF), w)

    def tile(k, off=0, w=WA):
        across, first = (D - NB * 2 * FF) // WA, NB * 2 * FF
        row, col = FF + k // across * R, first + k % across * WA + off
        return (pl.ds(pl.multiple_of(row, math.gcd(FF, R)), R), pl.ds(pl.multiple_of(col, math.gcd(first, WB)), w))

    def p_in(s, j, off=0, w=WA):
        return big[tile(s * 12 + j, off, w)].astype(F32)

    def p_tile(k):
        return big.at[tile(k)]

    def c_p(s):
        every = big.at[pl.ds(0, R), pl.ds(0, 12 * WA)]
        return copy(every, every, p_s, p_m.at[s], partner)

    def c_a2(s, o, m):
        return copy(a2s.at[o, m], a2r.at[s, o, m], a2_s.at[o, m], a2_m.at[s, o, m], fn(o))

    def c_a3(s, o):
        return copy(a3s.at[o], a3r.at[s, o], a3_s.at[o], a3_m.at[s, o], sn(o))

    def c_t1(o):
        return copy(t1s.at[o], t1r.at[o], t1_s.at[o], t1_m.at[o], zin_d)

    def c_t2(src, o):
        return copy(t2s.at[o], t2r.at[src, o], t2_s.at[o], t2_m.at[src, o], zin_d)

    def c_b1():
        return copy(b1s, b1r, b1_s, b1_m, zin_d)

    def c_b2(d):
        return copy(b2s, b2r.at[d], b2_s, b2_m.at[d], zin_d)

    def c_b3(d, to=up):
        return copy(b3s.at[d], b3r.at[d], b3_s.at[d], b3_m.at[d], to)

    def c_b4(o, m):
        return copy(b4s.at[m], b4r.at[m], b4_s.at[m], b4_m.at[m], fn(o))

    def c_b5(o):
        return copy(b5s, b5r, b5_s, b5_m, sn(o))

    def g_copies(kk):
        i, k, b = kk // NK, kk % NK, kk % NB
        rows, ks = pl.ds(pl.multiple_of(i * R, R), R), pl.ds(pl.multiple_of(k * KB, KB), KB)
        return (pltpu.make_async_copy(x_ref.at[rows, ks], xb.at[b], g_m.at[b, 0]),
                pltpu.make_async_copy(wg_ref.at[ks], big.at[weights(b, 0, FF)], g_m.at[b, 1]),
                pltpu.make_async_copy(wu_ref.at[ks], big.at[weights(b, FF, FF)], g_m.at[b, 2]))

    def wd_copy(k):
        core, m = jnp.where(k < 3, 1 - c, c), k % 3
        off = jnp.where(m < 2, col_a(core, m, 0), col_b(core, 0))
        cols = pl.ds(pl.multiple_of(off, 4 * WA), 4 * WA)
        return pltpu.make_async_copy(wdh_ref.at[:, cols], big.at[pl.ds(0, FF), cols], wd_m.at[k])

    def g_pieces(i, k0, k1):
        def step(k, _):
            kk = i * NK + k
            b = kk % NB
            for cp_ in g_copies(kk):
                cp_.wait()

            @pl.when(kk == NK - 1)
            def _():
                for p in range(6):
                    wd_copy(p).start()

            @pl.when((kk + NB - 1 < n * NK))
            def _():
                for cp_ in g_copies(kk + NB - 1):
                    cp_.start()

            @pl.when(k == 0)
            def _():
                acc[...] = jnp.zeros_like(acc)

            acc[...] += jnp.dot(xb[b], big[weights(b, 0, 2 * FF)], preferred_element_type=F32)
            return 0

        lax.fori_loop(k0, k1, step, 0)
        if k1 == NK:
            h[i % 3] = (jax.nn.silu(acc[:, :FF]) * acc[:, FF:]).astype(BF16)

    def s1(t):
        @pl.when(t >= 1)
        def _():
            c_p(0).wait_send()

        @pl.when(t >= 2)
        def _():
            pl.semaphore_wait(cp, 1)

        def step(j, _):
            @pl.when((t == 0) & (j % 2 == 0))
            def _():
                wd_copy(j // 2).wait()

            v = dot(t, jnp.where(j < 4, col_a(1 - c, 0, 2 * j), col_b(1 - c, 2 * j - 8)), 2 * WA, WA).astype(BF16)
            for k in range(2):
                m = j * 2 + k
                p_tile(24 + m)[...] = v[:, k * WA:(k + 1) * WA]
                copy(p_tile(24 + m), p_tile(t % 2 * 12 + m), p_s, p_m.at[t % 2], partner).start()
            return 0

        lax.fori_loop(0, 6, step, 0)

    def s2(t, m):
        def step(o, _):
            @pl.when(t >= 1)
            def _():
                c_a2(0, o, m).wait_send()

            if m == 0:
                @pl.when(t >= 2)
                def _():
                    pl.semaphore_wait(ca2.at[o], 1)

            g = gf(o) if m else gd
            v = dot(t, col_a(c, o, g), WA, WA) + p_in(t % 2, o * 4 + g)
            a2s[o, m] = v.astype(BF16)
            c_a2(t % 2, o, m).start()
            return 0

        lax.fori_loop(0, 2, step, 0)

    def s3(t):
        def step(o, _):
            @pl.when(t >= 1)
            def _():
                c_a3(0, o).wait_send()

            @pl.when(t >= 2)
            def _():
                pl.semaphore_wait(ca3.at[o], 1)

            c_a2(t % 2, o, 0).wait_recv()
            g = gs(o)
            v = dot(t, col_a(c, o, g), WA, WA) + p_in(t % 2, o * 4 + g) + a2r[t % 2, o, 0].astype(F32)
            a3s[o] = v.astype(BF16)
            c_a3(t % 2, o).start()
            return 0

        lax.fori_loop(0, 2, step, 0)

    def t1(t):
        @pl.when(t == 0)
        def _():
            for p in range(3, 6):
                wd_copy(p).wait()

        c_p(t % 2).wait_recv()

        @pl.when(outer)
        def _():
            @pl.when(t >= 1)
            def _():
                c_b1().wait_send()
                pl.semaphore_wait(cb1, 1)

            q = 3 - z
            b1s[...] = (dot(t, col_b(c, q), WA, WA) + p_in(t % 2, 8 + q)).astype(BF16)
            c_b1().start()

    def t2(t):
        @pl.when(t >= 1)
        def _():
            c_b2(0).wait_send()
            pl.semaphore_wait(cb2, 1)

        @pl.when(inner)
        def _():
            c_b1().wait_recv()

        q = (z + 2) % 4
        b2s[...] = (dot(t, col_b(c, q), WA, WA) + p_in(t % 2, 8 + q) + b1r[...].astype(F32)).astype(BF16)
        d = jnp.where(z < 2, 0, 1)
        c_b2(d).start()

        @pl.when(inner & (t + 1 < n))
        def _():
            signal(cb1, zout_d)

    def s4(u):
        for o in range(2):
            c_a3(u % 2, o).wait_recv()
            c_a2(u % 2, o, 1).wait_recv()

        @pl.when(outer)
        def _():
            def step(o, _):
                @pl.when(u >= 1)
                def _():
                    c_t1(o).wait_send()

                @pl.when((u >= 1) & (o == 0))
                def _():
                    pl.semaphore_wait(ct1, 1)

                t1s[o] = own_a(u, o, far).astype(BF16)
                c_t1(o).start()
                return 0

            lax.fori_loop(0, 2, step, 0)

    def own_a(u, o, half):
        s, ln = u % 2, lanes(half, H)
        return (dot(u, col_a(c, o, go, half), H, H) + p_in(s, o * 4 + go, half * H, H)
                + a2r[s, o, 1, :, ln].astype(F32) + a3r[s, o, :, ln].astype(F32))

    def s5(u):
        src = jnp.where(outer, 0, 1)

        def step(o, _):
            @pl.when(u >= 1)
            def _():
                c_t2(src, o).wait_send()

            @pl.when((u >= 1) & (o == 0))
            def _():
                pl.semaphore_wait(ct2, 1)

            @pl.when(inner)
            def _():
                c_t1(o).wait_recv()

            half = jnp.where(outer, near, far)
            t2s[o] = (own_a(u, o, half) + t1r[o].astype(F32)).astype(BF16)
            c_t2(src, o).start()
            return 0

        lax.fori_loop(0, 2, step, 0)

        @pl.when(inner & (u + 1 < n))
        def _():
            signal(ct1, zout_d)

    def rows(v):
        return pl.ds(pl.multiple_of(v * R, R), R)

    def win_a(u, o, g, half):
        return tot.at[rows(u), pl.ds(pl.multiple_of(col_a(c, o, g, half), H), H)]

    def win_b(u, q, g=0, w=WB):
        return tot.at[rows(u), pl.ds(pl.multiple_of(col_b(c, q, g), WB), w)]

    def fa_copies(u, o):
        w = win_a(u, o, go, near)
        f = fa.at[o]
        return ((f, w, fa_s.at[o, 0], g1_m.at[u], zout_d), (f, w, fa_s.at[o, 1], g1_m.at[u], zin_d),
                (f, w, fa_s.at[o, 2], g3_m.at[0, u], sn(o)), (f, w, fa_s.at[o, 3], g4_m.at[0, u], fn(o)),
                (f, w, fa_s.at[o, 4], g5_m.at[u], partner))

    def fa_done(u, o):
        for a in fa_copies(u, o):
            copy(*a).wait_send()
        pltpu.make_async_copy(fa.at[o], win_a(u, o, go, near), la_m.at[o]).wait()

    def s6(u):
        @pl.when(inner)
        def _():
            for o in range(2):
                for src in range(2):
                    c_t2(src, o).wait_recv()

            def step(o, _):
                @pl.when(u >= 1)
                def _():
                    fa_done(u, o)

                fa[o] = (own_a(u, o, near) + t2r[0, o].astype(F32) + t2r[1, o].astype(F32)).astype(BF16)
                pltpu.make_async_copy(fa.at[o], win_a(u, o, go, near), la_m.at[o]).start()
                for a in fa_copies(u, o):
                    copy(*a).start()
                return 0

            lax.fori_loop(0, 2, step, 0)

            @pl.when(u + 1 < n)
            def _():
                signal(ct2, zout_d)
                signal(ct2, zin_d)

        @pl.when(u + 2 < n)
        def _():
            for o in range(2):
                signal(ca2.at[o], fn(o))
                signal(ca3.at[o], sn(o))

    def t3(u):
        def step(d, _):
            ok = jnp.where(d == 0, up_ok, dn_ok)

            @pl.when(ok)
            def _():
                to = pick(d, up, down)

                @pl.when(u >= 1)
                def _():
                    c_b3(d, to).wait_send()
                    pl.semaphore_wait(cb3.at[d], 1)

                @pl.when(inner)
                def _():
                    c_b2(d).wait_recv()

                q = pick(d, zu, zd)
                b3s[d] = (dot(u, col_b(c, q), WA, WA) + p_in(u % 2, 8 + q) + b2r[d].astype(F32)).astype(BF16)
                c_b3(d, to).start()

            return 0

        lax.fori_loop(0, 2, step, 0)

        @pl.when(inner & (u + 1 < n))
        def _():
            signal(cb2, zout_d)
            signal(cb2, zin_d)

    def own_b(u, g):
        ln = lanes(g, WB)
        return (dot(u, col_b(c, z, g), WB, WB) + p_in(u % 2, 8 + z, g * WB, WB)
                + b3r[0, :, ln].astype(F32) + b3r[1, :, ln].astype(F32))

    def t4(u):
        @pl.when(dn_ok)
        def _():
            c_b3(0).wait_recv()

        @pl.when(up_ok)
        def _():
            c_b3(1).wait_recv()

        o = u % 2

        def step(m, _):
            @pl.when(u >= 1)
            def _():
                c_b4(o, m).wait_send()

            @pl.when((u >= 1) & (m == 0))
            def _():
                pl.semaphore_wait(cb4, 1)

            b4s[m] = own_b(u, jnp.where(m == 0, gd, gf(o))).astype(BF16)
            c_b4(o, m).start()
            return 0

        lax.fori_loop(0, 2, step, 0)

    def t5(u):
        o = u % 2

        @pl.when(u >= 1)
        def _():
            c_b5(o).wait_send()
            pl.semaphore_wait(cb5, 1)

        c_b4(o, 0).wait_recv()
        b5s[...] = (own_b(u, gs(o)) + b4r[0].astype(F32)).astype(BF16)
        c_b5(o).start()

    def fb_copies(u):
        w, o = win_b(u, z, go), u % 2
        return ((fb, w, fb_s.at[0], h1_m.at[u], sn(o)), (fb, w, fb_s.at[1], h2_m.at[0, u], fn(o)))

    def fb_local(u):
        return pltpu.make_async_copy(fb, win_b(u, z, go), lb_m)

    def t6(u):
        o = u % 2
        c_b4(o, 1).wait_recv()
        c_b5(o).wait_recv()

        @pl.when(u >= 1)
        def _():
            for a in fb_copies(u):
                copy(*a).wait_send()

        fb[...] = (own_b(u, go) + b4r[1].astype(F32) + b5r[...].astype(F32)).astype(BF16)
        fb_local(u).start()
        for a in fb_copies(u):
            copy(*a).start()

        @pl.when(u + 1 < n)
        def _():
            @pl.when(dn_ok)
            def _():
                signal(cb3.at[0], down)

            @pl.when(up_ok)
            def _():
                signal(cb3.at[1], up)

            signal(cb4, fn(1 - o))
            signal(cb5, sn(1 - o))

        @pl.when(u + 2 < n)
        def _():
            signal(cp, partner)

    def go_on(v, cond, k, src, rs, to):
        def make():
            return copy(src(v), src(v), q_s.at[k], rs(v), to)

        @pl.when(cond if cond is not True else v >= 0)
        def _():
            @pl.when(v >= 1)
            def _():
                make().wait_send()

            make().start()

    plan = []

    def op(group, cond, src, rs, to):
        plan.append((group, cond, len(plan), src, rs, to))

    def half_ops(group, cond, half, which):
        for o in range(2):
            w = functools.partial(lambda o, half, v: win_a(v, o, go, half), o, half)
            op(group, cond, w, functools.partial(lambda k, v: g3_m.at[k, v], which), sn(o))
            op(group, cond, w, functools.partial(lambda k, v: g4_m.at[k, v], which), fn(o))
            op(group, cond, w, lambda v: g5_m.at[v], partner)

    for o in range(2):
        op("q0", inner, functools.partial(lambda o, v: win_a(v, o, go, far), o), lambda v: g2_m.at[v], zout_d)
    half_ops("q0i", inner, far, 1)
    half_ops("q0o", outer, near, 0)
    half_ops("q1", outer, far, 1)
    for k, half in ((0, near), (1, far)):
        for o in range(2):
            w = functools.partial(lambda o, half, v: win_a(v, o, gs(o), half), o, half)
            op(f"q{2 + k}", True, w, functools.partial(lambda k, v: g4_m.at[2 + k, v], k), fn(o))
            op(f"q{2 + k}", True, w, lambda v: g5_m.at[v], partner)
    for o in range(2):
        for half in range(2):
            op("q4", True, functools.partial(lambda o, half, v: win_a(v, o, gf(o), half), o, half), lambda v: g5_m.at[v], partner)
            op("q5", True, functools.partial(lambda o, half, v: win_a(v, o, gd, half), o, half), lambda v: g5_m.at[v], partner)
    op("r0", True, lambda v: win_b(v, z, gs(v % 2)), lambda v: h2_m.at[1, v], None)
    block = lambda q: (lambda v: win_b(v, q, w=4 * WB))
    op("r1", up_ok, block(z), lambda v: hz_m.at[0, v], up)
    op("r1", dn_ok, block(z), lambda v: hz_m.at[1, v], down)
    op("r1", True, block(z), lambda v: h5_m.at[v], partner)
    zm2, zp2 = jnp.maximum(z - 2, 0), jnp.minimum(z + 2, 3)
    op("r2u", dn_ok & up_ok, block(zd), lambda v: hz_m.at[2, v], up)
    op("r2u", dn_ok, block(zd), lambda v: h5_m.at[v], partner)
    op("r2d", dn_ok & up_ok, block(zu), lambda v: hz_m.at[3, v], down)
    op("r2d", up_ok, block(zu), lambda v: h5_m.at[v], partner)
    op("r3u", z == 2, block(zm2), lambda v: hz_m.at[4, v], up)
    op("r3u", z >= 2, block(zm2), lambda v: h5_m.at[v], partner)
    op("r3d", z == 1, block(zp2), lambda v: hz_m.at[5, v], down)
    op("r3d", z <= 1, block(zp2), lambda v: h5_m.at[v], partner)
    op("r4", outer, block(3 - z), lambda v: h5_m.at[v], partner)

    def run(group, v):
        for g_, cond, k, src, rs, to in plan:
            if g_ == group:
                go_on(v, cond, k, src, rs, fn(v % 2) if to is None else to)

    def arrived(ref, sem):
        copy(ref, ref, q_s.at[0], sem, partner).wait_recv()

    def pair(v):
        return tot.at[rows(v), pl.ds(0, WA)]

    def q0a(v):
        arrived(pair(v), g1_m.at[v])
        run("q0", v)
        run("q0i", v)
        run("q0o", v)

    def q0b(v):
        arrived(win_b(v, 0), h1_m.at[v])
        run("r0", v)

    def q1a(v):
        @pl.when(outer)
        def _():
            arrived(pair(v), g2_m.at[v])

        run("q1", v)

    def q1b(v):
        fb_local(v).wait()
        for k in range(2):
            arrived(win_b(v, 0), h2_m.at[k, v])
        run("r1", v)

    def q2a(v):
        arrived(pair(v), g3_m.at[0, v])
        run("q2", v)

    def q3a(v):
        arrived(pair(v), g3_m.at[1, v])
        run("q3", v)

    def hop(v, up_there, down_there, k, groups):
        for there, kk, g in ((up_there, k, groups[0]), (down_there, k + 1, groups[1])):
            @pl.when(there)
            def _():
                arrived(win_b(v, 0, w=4 * WB), hz_m.at[kk, v])

            run(g, v)

    def q2b(v):
        hop(v, dn_ok, up_ok, 0, ("r2u", "r2d"))

    def q3b(v):
        hop(v, z >= 2, z <= 1, 2, ("r3u", "r3d"))

    def q4b(v):
        hop(v, z == 3, z == 0, 4, ("", "r4"))

    def q4a(v):
        for k in range(2):
            arrived(pair(v), g4_m.at[k, v])
        run("q4", v)

    def q5(v):
        for k in range(2):
            arrived(pair(v), g4_m.at[2 + k, v])
        run("q5", v)

    def all_here(v):
        arrived(tot.at[rows(v), pl.ds(0, 8 * WA)], g5_m.at[v])
        arrived(tot.at[rows(v), pl.ds(0, 16 * WB)], h5_m.at[v])

    def stage(v):
        all_here(v)
        pltpu.make_async_copy(tot.at[rows(v)], big.at[rows(v)], st_m.at[v]).start()

    for kk in range(NB - 1):
        for cp_ in g_copies(kk):
            cp_.start()

    barrier = pltpu.get_barrier_semaphore()
    for to in (partner, xn, yn):
        signal(barrier, to)
    pl.when(up_ok)(lambda: signal(barrier, up))
    pl.when(dn_ok)(lambda: signal(barrier, down))

    @pl.when(outer)
    def _():
        t1r[...] = jnp.zeros_like(t1r)
        b1r[...] = jnp.zeros_like(b1r)
        b2r[...] = jnp.zeros_like(b2r)

    @pl.when(z == 0)
    def _():
        b3r[0] = jnp.zeros_like(b3r[0])

    @pl.when(z == 3)
    def _():
        b3r[1] = jnp.zeros_like(b3r[1])

    g_pieces(0, 0, NK)
    pl.semaphore_wait(barrier, jnp.where(outer, 4, 5))
    s1(0)
    cut = [NK * k // 8 for k in range(9)]

    def slot(t, _):
        def at(i, f):
            @pl.when((i >= 0) & (i < n))
            def _():
                f(i)

        def g(a, b):
            at(t + 1, lambda i: g_pieces(i, cut[a], cut[b]))

        u, v, w, e = t - 1, t - 2, t - 3, t - 4
        at(v, q0a)
        at(t - 8, q4b)
        at(u, s4)
        g(0, 1)
        at(t, t1)
        at(u, t4)
        at(t, lambda i: s2(i, 0))
        at(u, s5)
        at(v, q1b)
        at(t - 7, q4a)
        g(1, 2)
        at(u, t5)
        at(t - 7, q3a)
        at(t, lambda i: s2(i, 1))
        g(2, 3)
        at(e, q2a)
        at(e, q3b)
        g(3, 4)
        at(t, t2)
        g(4, 6)
        at(u, s6)
        at(u, t6)
        at(t, s3)
        g(6, 8)
        at(v, q1a)
        at(t - 8, q5)
        at(t, t3)
        at(v, q2b)
        at(t + 1, s1)
        at(u, q0b)
        pl.when(t == n + 1)(lambda: c_p(0).wait_send())

        pl.when((t > n) & (t <= n + S))(lambda: stage(t - n - 1))

        return 0

    lax.fori_loop(0, n + 8, slot, 0)

    last = n - 1
    for o in range(2):
        for m in range(2):
            c_a2(0, o, m).wait_send()
        c_b4(0, o).wait_send()
        c_a3(0, o).wait_send()
        c_t2(0, o).wait_send()

        @pl.when(outer)
        def _():
            c_t1(o).wait_send()

        @pl.when(inner)
        def _():
            fa_done(last, o)

        @pl.when(up_ok if o == 0 else dn_ok)
        def _():
            c_b3(o).wait_send()

    @pl.when(outer)
    def _():
        c_b1().wait_send()

    c_b2(0).wait_send()
    c_b5(0).wait_send()
    for a in fb_copies(last):
        copy(*a).wait_send()
    for g_, cond, k, src, rs, to in plan:
        def done(k=k, src=src, rs=rs):
            copy(src(last), src(last), q_s.at[k], rs(last), partner).wait_send()

        if cond is True:
            done()
        else:
            pl.when(cond)(done)

    for v in range(S, n):
        all_here(v)
    for v in range(S):
        pltpu.make_async_copy(tot.at[rows(v)], big.at[rows(v)], st_m.at[v]).wait()


N_OPS = 2 + 6 * 3 + 8 + 8 + 1 + 3 + 8 + 1


def block_sums(cfg, x, w_gate, w_up, w_down):
    n, R, D, FF, WA, H, WB, KB = (cfg[k] for k in ("n", "R", "D", "FF", "WA", "H", "WB", "KB"))
    NB = 3
    vm = lambda *s: pltpu.VMEM(s, BF16)
    dma = lambda *s: pltpu.SemaphoreType.DMA(s) if s else pltpu.SemaphoreType.DMA
    reg = lambda *s: pltpu.SemaphoreType.REGULAR(s) if s else pltpu.SemaphoreType.REGULAR
    scratch = [
        vm(3, R, FF), vm(NB, R, KB), pltpu.VMEM((R, 2 * FF), F32),
        vm(2, 2, R, WA), vm(2, 2, 2, R, WA), vm(2, R, WA), vm(2, 2, R, WA),
        vm(2, R, H), vm(2, R, H), vm(2, R, H), vm(2, 2, R, H),
        vm(R, WA), vm(R, WA), vm(R, WA), vm(2, R, WA), vm(2, R, WA), vm(2, R, WA), vm(2, R, WB), vm(2, R, WB), vm(R, WB), vm(R, WB),
        vm(2, R, H), vm(R, WB),
        dma(6), dma(NB, 3), dma(staged(cfg)), dma(), dma(2), dma(2, 2), dma(2, 2, 2), dma(2), dma(2, 2), dma(2), dma(2), dma(2), dma(2, 2),
        dma(), dma(), dma(), dma(2), dma(2), dma(2), dma(2), dma(2), dma(), dma(),
        dma(2), dma(), dma(2, 5), dma(2), dma(N_OPS), dma(n), dma(n), dma(2, n), dma(4, n), dma(n), dma(n), dma(2, n), dma(6, n), dma(n),
        reg(), reg(2), reg(2), reg(), reg(), reg(), reg(), reg(2), reg(), reg(),
    ]
    hbm = pl.BlockSpec(memory_space=pl.ANY)
    return pl.pallas_call(
        functools.partial(body, cfg),
        name="mlp_sums",
        out_shape=(jax.ShapeDtypeStruct((n * R, D), BF16), vm(FF + KB, D)),
        in_specs=[hbm] * 4,
        out_specs=(hbm, pl.BlockSpec(memory_space=pltpu.VMEM)),
        scratch_shapes=scratch,
        compiler_params=pltpu.CompilerParams(collective_id=0, has_side_effects=True, vmem_limit_bytes=18_000_000),
    )(x, w_gate, w_up, w_down)


def place(cfg, total, big):
    n, R, D = (cfg[k] for k in ("n", "R", "D"))
    S = staged(cfg)
    K = 4

    def kernel(t_ref, big_ref, o_ref, buf, in_m, out_m, st_m):
        def whole(v):
            rows = pl.ds(v * R, R)
            return pltpu.make_async_copy(big_ref.at[rows], o_ref.at[rows], st_m.at[v])

        def piece(i):
            return pl.ds(S * R + i * (R // K), R // K)

        last = (n - S) * K
        ins = [pltpu.make_async_copy(t_ref.at[piece(i)], buf.at[i], in_m.at[i]) for i in range(last)]
        outs = [pltpu.make_async_copy(buf.at[i], o_ref.at[piece(i)], out_m.at[i]) for i in range(last)]
        for cp in ins:
            cp.start()
        for v in range(S):
            whole(v).start()
        for there, back in zip(ins, outs):
            there.wait()
            back.start()
        for cp in outs:
            cp.wait()
        for v in range(S):
            whole(v).wait()

    hbm, dma = pl.BlockSpec(memory_space=pl.ANY), pltpu.SemaphoreType.DMA
    parts = (n - S) * K
    return pl.pallas_call(
        kernel,
        name="place",
        out_shape=jax.ShapeDtypeStruct((n * R, D), BF16),
        in_specs=[hbm, pl.BlockSpec(memory_space=pltpu.VMEM)],
        out_specs=hbm,
        scratch_shapes=[pltpu.VMEM((parts, R // K, D), BF16), dma((parts,)), dma((parts,)), dma((S,))],
        compiler_params=pltpu.CompilerParams(vmem_limit_bytes=14_000_000),
    )(total, pltpu.with_memory_space_constraint(big, pltpu.VMEM))


def build(mesh, chunk, pieces):
    def step(x, w_gate, w_up, w_down):
        cfg = dims(x.shape[0], x.shape[1], w_gate.shape[1], chunk, pieces)
        return place(cfg, *block_sums(cfg, x, w_gate, w_up, w_down))

    return jax.shard_map(
        step,
        mesh=mesh,
        in_specs=(P("dp", None), P(None, "tp"), P(None, "tp"), P("tp", None)),
        out_specs=P("dp", None),
        check_vma=False,
    )


def solution(mesh):
    return build(mesh, 256, 12)
```

```python
import functools
import math

import jax
import jax.numpy as jnp
from jax import lax
from jax.experimental import pallas as pl
from jax.experimental.pallas import tpu as pltpu
from jax.sharding import PartitionSpec as P

F32 = jnp.float32
BF16 = jnp.bfloat16
MESH = pl.DeviceIdType.MESH


def dims(rows, d, ff, chunk, pieces):
    wa = d // 24
    return dict(n=rows // chunk, R=chunk, D=d, FF=ff, WA=wa, H=wa // 2, WB=wa // 4, NK=pieces, KB=d // pieces)


def staged(cfg):
    return min((cfg["FF"] + cfg["KB"]) // cfg["R"], cfg["n"] - 1)


def body(cfg, x_ref, wg_ref, wu_ref, wdh_ref, tot, big, h, xb, acc, a2s, a2r, a3s, a3r, t1s, t1r, t2s, t2r,
         b1s, b1r, b2s, b2r, b3s, b3r, b4s, b4r, b5s, b5r, fa, fb,
         wd_m, g_m, st_m, p_s, p_m, a2_s, a2_m, a3_s, a3_m, t1_s, t1_m, t2_s, t2_m, b1_s, b1_m, b2_s, b2_m, b3_s, b3_m, b4_s, b4_m, b5_s, b5_m,
         la_m, lb_m, fa_s, fb_s, q_s, g1_m, g2_m, g3_m, g4_m, g5_m, h1_m, h2_m, hz_m, h5_m,
         cp, ca2, ca3, ct1, ct2, cb1, cb2, cb3, cb4, cb5):
    n, R, D, FF, WA, H, WB, NK, KB = (cfg[k] for k in ("n", "R", "D", "FF", "WA", "H", "WB", "NK", "KB"))
    NB = xb.shape[0]
    S = staged(cfg)
    me = lax.axis_index("tp")
    dp = lax.axis_index("dp")
    x, y, z, c = me // 16, (me // 8) % 2, (me // 2) % 4, me % 2

    def dev(x, y, z, c):
        return (dp, ((x * 2 + y) * 4 + z) * 2 + c)

    outer = (z == 0) | (z == 3)
    inner = jnp.logical_not(outer)
    up_ok, dn_ok = z < 3, z > 0
    zu, zd = jnp.minimum(z + 1, 3), jnp.maximum(z - 1, 0)
    zin = jnp.where(outer, jnp.where(z == 0, 1, 2), 3 - z)
    zout = jnp.where(z < 2, 0, 3)
    near = jnp.where(z < 2, 0, 1)
    far = 1 - near
    partner = dev(x, y, z, 1 - c)
    xn, yn = dev(1 - x, y, z, c), dev(x, 1 - y, z, c)
    up, down, zin_d, zout_d = dev(x, y, zu, c), dev(x, y, zd, c), dev(x, y, zin, c), dev(x, y, zout, c)
    go, gx, gy, gd = x * 2 + y, (1 - x) * 2 + y, x * 2 + 1 - y, (1 - x) * 2 + 1 - y

    def pick(order, a, b):
        first = order == 0
        return jax.tree.map(lambda p, q: jnp.where(first, p, q), a, b)

    def fn(order):
        return pick(order, xn, yn)

    def sn(order):
        return pick(order, yn, xn)

    def gf(order):
        return pick(order, gx, gy)

    def gs(order):
        return pick(order, gy, gx)

    def copy(src, dst, ss, rs, to):
        return pltpu.make_async_remote_copy(src, dst, ss, rs, device_id=to, device_id_type=MESH)

    def signal(sem, to):
        pl.semaphore_signal(sem, inc=1, device_id=to, device_id_type=MESH)

    def col_a(core, order, g, half=0):
        return core * (8 * WA) + order * (4 * WA) + g * WA + half * H

    def col_b(core, q, g=0):
        return 16 * WA + core * (16 * WB) + q * (4 * WB) + g * WB

    def lanes(i, w):
        return pl.ds(pl.multiple_of(i * w, w), w)

    def dot(i, col, w, unit):
        return jnp.dot(h[i % 3], big[pl.ds(0, FF), pl.ds(pl.multiple_of(col, unit), w)], preferred_element_type=F32)

    def weights(b, off, w):
        return pl.ds(FF, KB), pl.ds(pl.multiple_of(b * 2 * FF + off, FF), w)

    def tile(k, off=0, w=WA):
        across, first = (D - NB * 2 * FF) // WA, NB * 2 * FF
        row, col = FF + k // across * R, first + k % across * WA + off
        return (pl.ds(pl.multiple_of(row, math.gcd(FF, R)), R), pl.ds(pl.multiple_of(col, math.gcd(first, WB)), w))

    def p_in(s, j, off=0, w=WA):
        return big[tile(s * 12 + j, off, w)].astype(F32)

    def p_tile(k):
        return big.at[tile(k)]

    def c_p(s):
        every = big.at[pl.ds(0, R), pl.ds(0, 12 * WA)]
        return copy(every, every, p_s, p_m.at[s], partner)

    def c_a2(s, o, m):
        return copy(a2s.at[o, m], a2r.at[s, o, m], a2_s.at[o, m], a2_m.at[s, o, m], fn(o))

    def c_a3(s, o):
        return copy(a3s.at[o], a3r.at[s, o], a3_s.at[o], a3_m.at[s, o], sn(o))

    def c_t1(o):
        return copy(t1s.at[o], t1r.at[o], t1_s.at[o], t1_m.at[o], zin_d)

    def c_t2(src, o):
        return copy(t2s.at[o], t2r.at[src, o], t2_s.at[o], t2_m.at[src, o], zin_d)

    def c_b1():
        return copy(b1s, b1r, b1_s, b1_m, zin_d)

    def c_b2(d):
        return copy(b2s, b2r.at[d], b2_s, b2_m.at[d], zin_d)

    def c_b3(d, to=up):
        return copy(b3s.at[d], b3r.at[d], b3_s.at[d], b3_m.at[d], to)

    def c_b4(o, m):
        return copy(b4s.at[m], b4r.at[m], b4_s.at[m], b4_m.at[m], fn(o))

    def c_b5(o):
        return copy(b5s, b5r, b5_s, b5_m, sn(o))

    def g_copies(kk):
        i, k, b = kk // NK, kk % NK, kk % NB
        rows, ks = pl.ds(pl.multiple_of(i * R, R), R), pl.ds(pl.multiple_of(k * KB, KB), KB)
        return (pltpu.make_async_copy(x_ref.at[rows, ks], xb.at[b], g_m.at[b, 0]),
                pltpu.make_async_copy(wg_ref.at[ks], big.at[weights(b, 0, FF)], g_m.at[b, 1]),
                pltpu.make_async_copy(wu_ref.at[ks], big.at[weights(b, FF, FF)], g_m.at[b, 2]))

    def wd_copy(k):
        core, m = jnp.where(k < 3, 1 - c, c), k % 3
        off = jnp.where(m < 2, col_a(core, m, 0), col_b(core, 0))
        cols = pl.ds(pl.multiple_of(off, 4 * WA), 4 * WA)
        return pltpu.make_async_copy(wdh_ref.at[:, cols], big.at[pl.ds(0, FF), cols], wd_m.at[k])

    def g_pieces(i, k0, k1):
        def step(k, _):
            kk = i * NK + k
            b = kk % NB
            for cp_ in g_copies(kk):
                cp_.wait()

            @pl.when(kk == NK - 1)
            def _():
                for p in range(6):
                    wd_copy(p).start()

            @pl.when((kk + NB - 1 < n * NK))
            def _():
                for cp_ in g_copies(kk + NB - 1):
                    cp_.start()

            @pl.when(k == 0)
            def _():
                acc[...] = jnp.zeros_like(acc)

            acc[...] += jnp.dot(xb[b], big[weights(b, 0, 2 * FF)], preferred_element_type=F32)
            return 0

        lax.fori_loop(k0, k1, step, 0)
        if k1 == NK:
            h[i % 3] = (jax.nn.silu(acc[:, :FF]) * acc[:, FF:]).astype(BF16)

    def s1(t):
        @pl.when(t >= 1)
        def _():
            c_p(0).wait_send()

        @pl.when(t >= 2)
        def _():
            pl.semaphore_wait(cp, 1)

        def step(j, _):
            @pl.when((t == 0) & (j % 2 == 0))
            def _():
                wd_copy(j // 2).wait()

            v = dot(t, jnp.where(j < 4, col_a(1 - c, 0, 2 * j), col_b(1 - c, 2 * j - 8)), 2 * WA, WA).astype(BF16)
            for k in range(2):
                m = j * 2 + k
                p_tile(24 + m)[...] = v[:, k * WA:(k + 1) * WA]
                copy(p_tile(24 + m), p_tile(t % 2 * 12 + m), p_s, p_m.at[t % 2], partner).start()
            return 0

        lax.fori_loop(0, 6, step, 0)

    def s2(t, m):
        def step(o, _):
            @pl.when(t >= 1)
            def _():
                c_a2(0, o, m).wait_send()

            if m == 0:
                @pl.when(t >= 2)
                def _():
                    pl.semaphore_wait(ca2.at[o], 1)

            g = gf(o) if m else gd
            v = dot(t, col_a(c, o, g), WA, WA) + p_in(t % 2, o * 4 + g)
            a2s[o, m] = v.astype(BF16)
            c_a2(t % 2, o, m).start()
            return 0

        lax.fori_loop(0, 2, step, 0)

    def s3(t):
        def step(o, _):
            @pl.when(t >= 1)
            def _():
                c_a3(0, o).wait_send()

            @pl.when(t >= 2)
            def _():
                pl.semaphore_wait(ca3.at[o], 1)

            c_a2(t % 2, o, 0).wait_recv()
            g = gs(o)
            v = dot(t, col_a(c, o, g), WA, WA) + p_in(t % 2, o * 4 + g) + a2r[t % 2, o, 0].astype(F32)
            a3s[o] = v.astype(BF16)
            c_a3(t % 2, o).start()
            return 0

        lax.fori_loop(0, 2, step, 0)

    def t1(t):
        @pl.when(t == 0)
        def _():
            for p in range(3, 6):
                wd_copy(p).wait()

        c_p(t % 2).wait_recv()

        @pl.when(outer)
        def _():
            @pl.when(t >= 1)
            def _():
                c_b1().wait_send()
                pl.semaphore_wait(cb1, 1)

            q = 3 - z
            b1s[...] = (dot(t, col_b(c, q), WA, WA) + p_in(t % 2, 8 + q)).astype(BF16)
            c_b1().start()

    def t2(t):
        @pl.when(t >= 1)
        def _():
            c_b2(0).wait_send()
            pl.semaphore_wait(cb2, 1)

        @pl.when(inner)
        def _():
            c_b1().wait_recv()

        q = (z + 2) % 4
        b2s[...] = (dot(t, col_b(c, q), WA, WA) + p_in(t % 2, 8 + q) + b1r[...].astype(F32)).astype(BF16)
        d = jnp.where(z < 2, 0, 1)
        c_b2(d).start()

        @pl.when(inner & (t + 1 < n))
        def _():
            signal(cb1, zout_d)

    def s4(u):
        for o in range(2):
            c_a3(u % 2, o).wait_recv()
            c_a2(u % 2, o, 1).wait_recv()

        @pl.when(outer)
        def _():
            def step(o, _):
                @pl.when(u >= 1)
                def _():
                    c_t1(o).wait_send()

                @pl.when((u >= 1) & (o == 0))
                def _():
                    pl.semaphore_wait(ct1, 1)

                t1s[o] = own_a(u, o, far).astype(BF16)
                c_t1(o).start()
                return 0

            lax.fori_loop(0, 2, step, 0)

    def own_a(u, o, half):
        s, ln = u % 2, lanes(half, H)
        return (dot(u, col_a(c, o, go, half), H, H) + p_in(s, o * 4 + go, half * H, H)
                + a2r[s, o, 1, :, ln].astype(F32) + a3r[s, o, :, ln].astype(F32))

    def s5(u):
        src = jnp.where(outer, 0, 1)

        def step(o, _):
            @pl.when(u >= 1)
            def _():
                c_t2(src, o).wait_send()

            @pl.when((u >= 1) & (o == 0))
            def _():
                pl.semaphore_wait(ct2, 1)

            @pl.when(inner)
            def _():
                c_t1(o).wait_recv()

            half = jnp.where(outer, near, far)
            t2s[o] = (own_a(u, o, half) + t1r[o].astype(F32)).astype(BF16)
            c_t2(src, o).start()
            return 0

        lax.fori_loop(0, 2, step, 0)

        @pl.when(inner & (u + 1 < n))
        def _():
            signal(ct1, zout_d)

    def rows(v):
        return pl.ds(pl.multiple_of(v * R, R), R)

    def win_a(u, o, g, half):
        return tot.at[rows(u), pl.ds(pl.multiple_of(col_a(c, o, g, half), H), H)]

    def win_b(u, q, g=0, w=WB):
        return tot.at[rows(u), pl.ds(pl.multiple_of(col_b(c, q, g), WB), w)]

    def fa_copies(u, o):
        w = win_a(u, o, go, near)
        f = fa.at[o]
        return ((f, w, fa_s.at[o, 0], g1_m.at[u], zout_d), (f, w, fa_s.at[o, 1], g1_m.at[u], zin_d),
                (f, w, fa_s.at[o, 2], g3_m.at[0, u], sn(o)), (f, w, fa_s.at[o, 3], g4_m.at[0, u], fn(o)),
                (f, w, fa_s.at[o, 4], g5_m.at[u], partner))

    def fa_done(u, o):
        for a in fa_copies(u, o):
            copy(*a).wait_send()
        pltpu.make_async_copy(fa.at[o], win_a(u, o, go, near), la_m.at[o]).wait()

    def s6(u):
        @pl.when(inner)
        def _():
            for o in range(2):
                for src in range(2):
                    c_t2(src, o).wait_recv()

            def step(o, _):
                @pl.when(u >= 1)
                def _():
                    fa_done(u, o)

                fa[o] = (own_a(u, o, near) + t2r[0, o].astype(F32) + t2r[1, o].astype(F32)).astype(BF16)
                pltpu.make_async_copy(fa.at[o], win_a(u, o, go, near), la_m.at[o]).start()
                for a in fa_copies(u, o):
                    copy(*a).start()
                return 0

            lax.fori_loop(0, 2, step, 0)

            @pl.when(u + 1 < n)
            def _():
                signal(ct2, zout_d)
                signal(ct2, zin_d)

        @pl.when(u + 2 < n)
        def _():
            for o in range(2):
                signal(ca2.at[o], fn(o))
                signal(ca3.at[o], sn(o))

    def t3(u):
        def step(d, _):
            ok = jnp.where(d == 0, up_ok, dn_ok)

            @pl.when(ok)
            def _():
                to = pick(d, up, down)

                @pl.when(u >= 1)
                def _():
                    c_b3(d, to).wait_send()
                    pl.semaphore_wait(cb3.at[d], 1)

                @pl.when(inner)
                def _():
                    c_b2(d).wait_recv()

                q = pick(d, zu, zd)
                b3s[d] = (dot(u, col_b(c, q), WA, WA) + p_in(u % 2, 8 + q) + b2r[d].astype(F32)).astype(BF16)
                c_b3(d, to).start()

            return 0

        lax.fori_loop(0, 2, step, 0)

        @pl.when(inner & (u + 1 < n))
        def _():
            signal(cb2, zout_d)
            signal(cb2, zin_d)

    def own_b(u, g):
        ln = lanes(g, WB)
        return (dot(u, col_b(c, z, g), WB, WB) + p_in(u % 2, 8 + z, g * WB, WB)
                + b3r[0, :, ln].astype(F32) + b3r[1, :, ln].astype(F32))

    def t4(u):
        @pl.when(dn_ok)
        def _():
            c_b3(0).wait_recv()

        @pl.when(up_ok)
        def _():
            c_b3(1).wait_recv()

        o = u % 2

        def step(m, _):
            @pl.when(u >= 1)
            def _():
                c_b4(o, m).wait_send()

            @pl.when((u >= 1) & (m == 0))
            def _():
                pl.semaphore_wait(cb4, 1)

            b4s[m] = own_b(u, jnp.where(m == 0, gd, gf(o))).astype(BF16)
            c_b4(o, m).start()
            return 0

        lax.fori_loop(0, 2, step, 0)

    def t5(u):
        o = u % 2

        @pl.when(u >= 1)
        def _():
            c_b5(o).wait_send()
            pl.semaphore_wait(cb5, 1)

        c_b4(o, 0).wait_recv()
        b5s[...] = (own_b(u, gs(o)) + b4r[0].astype(F32)).astype(BF16)
        c_b5(o).start()

    def fb_copies(u):
        w, o = win_b(u, z, go), u % 2
        return ((fb, w, fb_s.at[0], h1_m.at[u], sn(o)), (fb, w, fb_s.at[1], h2_m.at[0, u], fn(o)))

    def fb_local(u):
        return pltpu.make_async_copy(fb, win_b(u, z, go), lb_m)

    def t6(u):
        o = u % 2
        c_b4(o, 1).wait_recv()
        c_b5(o).wait_recv()

        @pl.when(u >= 1)
        def _():
            for a in fb_copies(u):
                copy(*a).wait_send()

        fb[...] = (own_b(u, go) + b4r[1].astype(F32) + b5r[...].astype(F32)).astype(BF16)
        fb_local(u).start()
        for a in fb_copies(u):
            copy(*a).start()

        @pl.when(u + 1 < n)
        def _():
            @pl.when(dn_ok)
            def _():
                signal(cb3.at[0], down)

            @pl.when(up_ok)
            def _():
                signal(cb3.at[1], up)

            signal(cb4, fn(1 - o))
            signal(cb5, sn(1 - o))

        @pl.when(u + 2 < n)
        def _():
            signal(cp, partner)

    def go_on(v, cond, k, src, rs, to):
        def make():
            return copy(src(v), src(v), q_s.at[k], rs(v), to)

        @pl.when(cond if cond is not True else v >= 0)
        def _():
            @pl.when(v >= 1)
            def _():
                make().wait_send()

            make().start()

    plan = []

    def op(group, cond, src, rs, to):
        plan.append((group, cond, len(plan), src, rs, to))

    def half_ops(group, cond, half, which):
        for o in range(2):
            w = functools.partial(lambda o, half, v: win_a(v, o, go, half), o, half)
            op(group, cond, w, functools.partial(lambda k, v: g3_m.at[k, v], which), sn(o))
            op(group, cond, w, functools.partial(lambda k, v: g4_m.at[k, v], which), fn(o))
            op(group, cond, w, lambda v: g5_m.at[v], partner)

    for o in range(2):
        op("q0", inner, functools.partial(lambda o, v: win_a(v, o, go, far), o), lambda v: g2_m.at[v], zout_d)
    half_ops("q0i", inner, far, 1)
    half_ops("q0o", outer, near, 0)
    half_ops("q1", outer, far, 1)
    for k, half in ((0, near), (1, far)):
        for o in range(2):
            w = functools.partial(lambda o, half, v: win_a(v, o, gs(o), half), o, half)
            op(f"q{2 + k}", True, w, functools.partial(lambda k, v: g4_m.at[2 + k, v], k), fn(o))
            op(f"q{2 + k}", True, w, lambda v: g5_m.at[v], partner)
    for o in range(2):
        for half in range(2):
            op("q4", True, functools.partial(lambda o, half, v: win_a(v, o, gf(o), half), o, half), lambda v: g5_m.at[v], partner)
            op("q5", True, functools.partial(lambda o, half, v: win_a(v, o, gd, half), o, half), lambda v: g5_m.at[v], partner)
    op("r0", True, lambda v: win_b(v, z, gs(v % 2)), lambda v: h2_m.at[1, v], None)
    block = lambda q: (lambda v: win_b(v, q, w=4 * WB))
    op("r1", up_ok, block(z), lambda v: hz_m.at[0, v], up)
    op("r1", dn_ok, block(z), lambda v: hz_m.at[1, v], down)
    op("r1", True, block(z), lambda v: h5_m.at[v], partner)
    zm2, zp2 = jnp.maximum(z - 2, 0), jnp.minimum(z + 2, 3)
    op("r2u", dn_ok & up_ok, block(zd), lambda v: hz_m.at[2, v], up)
    op("r2u", dn_ok, block(zd), lambda v: h5_m.at[v], partner)
    op("r2d", dn_ok & up_ok, block(zu), lambda v: hz_m.at[3, v], down)
    op("r2d", up_ok, block(zu), lambda v: h5_m.at[v], partner)
    op("r3u", z == 2, block(zm2), lambda v: hz_m.at[4, v], up)
    op("r3u", z >= 2, block(zm2), lambda v: h5_m.at[v], partner)
    op("r3d", z == 1, block(zp2), lambda v: hz_m.at[5, v], down)
    op("r3d", z <= 1, block(zp2), lambda v: h5_m.at[v], partner)
    op("r4", outer, block(3 - z), lambda v: h5_m.at[v], partner)

    def run(group, v):
        for g_, cond, k, src, rs, to in plan:
            if g_ == group:
                go_on(v, cond, k, src, rs, fn(v % 2) if to is None else to)

    def arrived(ref, sem):
        copy(ref, ref, q_s.at[0], sem, partner).wait_recv()

    def pair(v):
        return tot.at[rows(v), pl.ds(0, WA)]

    def q0a(v):
        arrived(pair(v), g1_m.at[v])
        run("q0", v)
        run("q0i", v)
        run("q0o", v)

    def q0b(v):
        arrived(win_b(v, 0), h1_m.at[v])
        run("r0", v)

    def q1a(v):
        @pl.when(outer)
        def _():
            arrived(pair(v), g2_m.at[v])

        run("q1", v)

    def q1b(v):
        fb_local(v).wait()
        for k in range(2):
            arrived(win_b(v, 0), h2_m.at[k, v])
        run("r1", v)

    def q2a(v):
        arrived(pair(v), g3_m.at[0, v])
        run("q2", v)

    def q3a(v):
        arrived(pair(v), g3_m.at[1, v])
        run("q3", v)

    def hop(v, up_there, down_there, k, groups):
        for there, kk, g in ((up_there, k, groups[0]), (down_there, k + 1, groups[1])):
            @pl.when(there)
            def _():
                arrived(win_b(v, 0, w=4 * WB), hz_m.at[kk, v])

            run(g, v)

    def q2b(v):
        hop(v, dn_ok, up_ok, 0, ("r2u", "r2d"))

    def q3b(v):
        hop(v, z >= 2, z <= 1, 2, ("r3u", "r3d"))

    def q4b(v):
        hop(v, z == 3, z == 0, 4, ("", "r4"))

    def q4a(v):
        for k in range(2):
            arrived(pair(v), g4_m.at[k, v])
        run("q4", v)

    def q5(v):
        for k in range(2):
            arrived(pair(v), g4_m.at[2 + k, v])
        run("q5", v)

    def all_here(v):
        arrived(tot.at[rows(v), pl.ds(0, 8 * WA)], g5_m.at[v])
        arrived(tot.at[rows(v), pl.ds(0, 16 * WB)], h5_m.at[v])

    def stage(v):
        all_here(v)
        pltpu.make_async_copy(tot.at[rows(v)], big.at[rows(v)], st_m.at[v]).start()

    for kk in range(NB - 1):
        for cp_ in g_copies(kk):
            cp_.start()

    barrier = pltpu.get_barrier_semaphore()
    for to in (partner, xn, yn):
        signal(barrier, to)
    pl.when(up_ok)(lambda: signal(barrier, up))
    pl.when(dn_ok)(lambda: signal(barrier, down))

    @pl.when(outer)
    def _():
        t1r[...] = jnp.zeros_like(t1r)
        b1r[...] = jnp.zeros_like(b1r)
        b2r[...] = jnp.zeros_like(b2r)

    @pl.when(z == 0)
    def _():
        b3r[0] = jnp.zeros_like(b3r[0])

    @pl.when(z == 3)
    def _():
        b3r[1] = jnp.zeros_like(b3r[1])

    g_pieces(0, 0, NK)
    pl.semaphore_wait(barrier, jnp.where(outer, 4, 5))
    s1(0)
    cut = [NK * k // 8 for k in range(9)]

    def slot(t, _):
        def at(i, f):
            @pl.when((i >= 0) & (i < n))
            def _():
                f(i)

        def g(a, b):
            at(t + 1, lambda i: g_pieces(i, cut[a], cut[b]))

        u, v, w, e = t - 1, t - 2, t - 3, t - 4
        at(v, q0a)
        at(t - 8, q4b)
        at(u, s4)
        g(0, 1)
        at(t, t1)
        at(u, t4)
        at(t, lambda i: s2(i, 0))
        at(u, s5)
        at(v, q1b)
        at(t - 7, q4a)
        g(1, 2)
        at(u, t5)
        at(t - 7, q3a)
        at(t, lambda i: s2(i, 1))
        g(2, 3)
        at(e, q2a)
        at(e, q3b)
        g(3, 4)
        at(t, t2)
        g(4, 6)
        at(u, s6)
        at(u, t6)
        at(t, s3)
        g(6, 8)
        at(v, q1a)
        at(t - 8, q5)
        at(t, t3)
        at(v, q2b)
        at(t + 1, s1)
        at(u, q0b)
        return 0

    lax.fori_loop(0, n + 1, slot, 0)
    c_p(0).wait_send()
    stages = {f.__name__: f for f in (q0a, q1a, q1b, q2a, q2b, q3a, q3b, q4a, q4b, q5, stage)}
    for name in ("q0a7", "stage0", "q4b1", "q3a2", "q3a3", "q4a2", "q1b7", "q4b2", "q3b5", "q4b3", "q2a5", "q3a4",
            "q2a6", "q51", "q52", "stage1", "q1a7", "q4a3", "q3b6", "q4a4", "q3a5", "q3a6", "q4b4", "q4b5",
            "q4a5", "q2b7", "q2a7", "q53", "stage2", "q54", "stage3", "q55", "stage4", "q4b6", "q3a7", "q4a6",
            "q3b7", "q56", "stage5", "q57", "q4b7", "q4a7", "stage6"):
        stages[name[:-1]](jnp.int32(int(name[-1])))

    last = n - 1
    for o in range(2):
        for m in range(2):
            c_a2(0, o, m).wait_send()
        c_b4(0, o).wait_send()
        c_a3(0, o).wait_send()
        c_t2(0, o).wait_send()

        @pl.when(outer)
        def _():
            c_t1(o).wait_send()

        @pl.when(inner)
        def _():
            fa_done(last, o)

        @pl.when(up_ok if o == 0 else dn_ok)
        def _():
            c_b3(o).wait_send()

    @pl.when(outer)
    def _():
        c_b1().wait_send()

    c_b2(0).wait_send()
    c_b5(0).wait_send()
    for a in fb_copies(last):
        copy(*a).wait_send()
    for g_, cond, k, src, rs, to in plan:
        def done(k=k, src=src, rs=rs):
            copy(src(last), src(last), q_s.at[k], rs(last), partner).wait_send()

        if cond is True:
            done()
        else:
            pl.when(cond)(done)

    for v in range(S, n):
        all_here(v)
    for v in range(S):
        pltpu.make_async_copy(tot.at[rows(v)], big.at[rows(v)], st_m.at[v]).wait()


N_OPS = 2 + 6 * 3 + 8 + 8 + 1 + 3 + 8 + 1


def block_sums(cfg, x, w_gate, w_up, w_down):
    n, R, D, FF, WA, H, WB, KB = (cfg[k] for k in ("n", "R", "D", "FF", "WA", "H", "WB", "KB"))
    NB = 3
    vm = lambda *s: pltpu.VMEM(s, BF16)
    dma = lambda *s: pltpu.SemaphoreType.DMA(s) if s else pltpu.SemaphoreType.DMA
    reg = lambda *s: pltpu.SemaphoreType.REGULAR(s) if s else pltpu.SemaphoreType.REGULAR
    scratch = [
        vm(3, R, FF), vm(NB, R, KB), pltpu.VMEM((R, 2 * FF), F32),
        vm(2, 2, R, WA), vm(2, 2, 2, R, WA), vm(2, R, WA), vm(2, 2, R, WA),
        vm(2, R, H), vm(2, R, H), vm(2, R, H), vm(2, 2, R, H),
        vm(R, WA), vm(R, WA), vm(R, WA), vm(2, R, WA), vm(2, R, WA), vm(2, R, WA), vm(2, R, WB), vm(2, R, WB), vm(R, WB), vm(R, WB),
        vm(2, R, H), vm(R, WB),
        dma(6), dma(NB, 3), dma(staged(cfg)), dma(), dma(2), dma(2, 2), dma(2, 2, 2), dma(2), dma(2, 2), dma(2), dma(2), dma(2), dma(2, 2),
        dma(), dma(), dma(), dma(2), dma(2), dma(2), dma(2), dma(2), dma(), dma(),
        dma(2), dma(), dma(2, 5), dma(2), dma(N_OPS), dma(n), dma(n), dma(2, n), dma(4, n), dma(n), dma(n), dma(2, n), dma(6, n), dma(n),
        reg(), reg(2), reg(2), reg(), reg(), reg(), reg(), reg(2), reg(), reg(),
    ]
    hbm = pl.BlockSpec(memory_space=pl.ANY)
    return pl.pallas_call(
        functools.partial(body, cfg),
        name="mlp_sums",
        out_shape=(jax.ShapeDtypeStruct((n * R, D), BF16), vm(FF + KB, D)),
        in_specs=[hbm] * 4,
        out_specs=(hbm, pl.BlockSpec(memory_space=pltpu.VMEM)),
        scratch_shapes=scratch,
        compiler_params=pltpu.CompilerParams(collective_id=0, has_side_effects=True, vmem_limit_bytes=18_000_000),
    )(x, w_gate, w_up, w_down)


def place(cfg, total, big):
    n, R, D = (cfg[k] for k in ("n", "R", "D"))
    S = staged(cfg)
    K = 4

    def kernel(t_ref, big_ref, o_ref, buf, in_m, out_m, st_m):
        def whole(v):
            rows = pl.ds(v * R, R)
            return pltpu.make_async_copy(big_ref.at[rows], o_ref.at[rows], st_m.at[v])

        def piece(i):
            return pl.ds(S * R + i * (R // K), R // K)

        last = (n - S) * K
        ins = [pltpu.make_async_copy(t_ref.at[piece(i)], buf.at[i], in_m.at[i]) for i in range(last)]
        outs = [pltpu.make_async_copy(buf.at[i], o_ref.at[piece(i)], out_m.at[i]) for i in range(last)]
        for cp in ins:
            cp.start()
        for v in range(S):
            whole(v).start()
        for there, back in zip(ins, outs):
            there.wait()
            back.start()
        for cp in outs:
            cp.wait()
        for v in range(S):
            whole(v).wait()

    hbm, dma = pl.BlockSpec(memory_space=pl.ANY), pltpu.SemaphoreType.DMA
    parts = (n - S) * K
    return pl.pallas_call(
        kernel,
        name="place",
        out_shape=jax.ShapeDtypeStruct((n * R, D), BF16),
        in_specs=[hbm, pl.BlockSpec(memory_space=pltpu.VMEM)],
        out_specs=hbm,
        scratch_shapes=[pltpu.VMEM((parts, R // K, D), BF16), dma((parts,)), dma((parts,)), dma((S,))],
        compiler_params=pltpu.CompilerParams(vmem_limit_bytes=14_000_000),
    )(total, pltpu.with_memory_space_constraint(big, pltpu.VMEM))


def build(mesh, chunk, pieces):
    def step(x, w_gate, w_up, w_down):
        cfg = dims(x.shape[0], x.shape[1], w_gate.shape[1], chunk, pieces)
        return place(cfg, *block_sums(cfg, x, w_gate, w_up, w_down))

    return jax.shard_map(
        step,
        mesh=mesh,
        in_specs=(P("dp", None), P(None, "tp"), P(None, "tp"), P("tp", None)),
        out_specs=P("dp", None),
        check_vma=False,
    )


def solution(mesh):
    return build(mesh, 256, 12)
```
